32 devices in a mesh: layer: 4 (over z), leaf: 8 (over y, x, core).
Axes of the slice: x: 2, y: 2, z: 4, core: 2. Of those that a mesh axis runs over, the one named last changes fastest.
Arguments:
- right_side: bfloat16 [4, 2, 32, 8192], P('layer', None, None, 'leaf'), may hold values from -6 to 6
- near_blocks: bfloat16 [4, 3, 2, 8192, 256], P('layer', None, None, 'leaf'), may hold values from -0.21875 to 0.21875
- right_bases: bfloat16 [4, 2, 2, 16, 8192], P('layer', None, None, None, 'leaf'), may hold values from -0.125 to 0.125
- left_bases: bfloat16 [4, 2, 2, 16, 8192], P('layer', None, None, None, 'leaf'), may hold values from -1 to 1
- coupling: bfloat16 [4, 8192], P('layer', 'leaf'), may hold values from 0.25 to 0.69921875
- ranks: int32 [4, 6], P('layer'), may hold values from 8 to 16
Outputs:
- swept: bfloat16 [4, 2, 32, 8192], P('layer', None, None, 'leaf')
The draws below stay inside these ranges and needn't reach their ends.
Inputs may be any that keep to these rules, and one draw needn't show every extreme that they name: ranks[k, s] is the rank in use of layer k's far block that maps into cluster s at level 0 (s = 0, 1) or cluster s - 2 at level 1 (s = 2 to 5).
All inputs are finite; a program needn't handle non-finite values.
Results may differ from the reference program's by a relative error of at most 0.035.
Values may be sent and summed in bfloat16 or wider, within the bound.
A program may use at most 64 MiB of HBM per device.

```python
import math
import jax
import jax.numpy as jnp
from jax import lax

CELLS = 256
RANK = 16
RHS = 32
PLANE = 8192
N_LAYER = 4


def touch_ends(drawn, stream_key, low, top_value):
    place = [jax.random.randint(jax.random.fold_in(stream_key, axis), (), 0, length) for axis, length in enumerate(drawn.shape)]
    longest = drawn.shape.index(max(drawn.shape))
    next_to = place[:longest] + [(place[longest] + 1) % drawn.shape[longest]] + place[longest + 1:]
    return drawn.at[tuple(place)].set(low).at[tuple(next_to)].set(top_value)


def levels(own_key, dims, shards, low, largest):
    gain = 1.0
    for position, blocks in shards:
        draws = jax.random.uniform(jax.random.fold_in(jax.random.fold_in(own_key, 6), position), (blocks,), jnp.float32, low / len(shards), largest / len(shards))
        gain = gain * jnp.repeat(jnp.exp(draws), dims[position] // blocks).reshape((-1,) + (1,) * (len(dims) - 1 - position))
    return gain


def centred(own_key, extent, spread, limit, shards=(), held_as=jnp.bfloat16):
    factor_of = levels(own_key, extent, shards, -0.22, 0.18) if shards else 1.0
    array = jax.random.normal(own_key, extent, jnp.float32) * spread * factor_of
    return jnp.minimum(jnp.maximum(array, -limit), limit).astype(held_as)


def setup_inputs(seed: int = 0) -> dict:
    key_list = jax.random.split(jax.random.key(seed), 7)
    return {
        "right_side": centred(key_list[0], (N_LAYER, 2, RHS, PLANE), 1.0, 6.0, ((0, 4), (3, 8))),
        "near_blocks": centred(key_list[1], (N_LAYER, 3, 2, PLANE, CELLS), (3 * CELLS) ** -0.5, 0.21875, ((0, 4), (3, 8))),
        "right_bases": centred(key_list[2], (N_LAYER, 2, 2, RANK, PLANE), (PLANE // 4) ** -0.5, 0.125, ((0, 4), (4, 8))),
        "left_bases": centred(key_list[3], (N_LAYER, 2, 2, RANK, PLANE), (2 * RANK) ** -0.5, 1.0, ((0, 4), (4, 8))),
        "coupling": jnp.clip(jnp.exp(math.log(0.69921875) - 1.0285027 * jax.random.uniform(key_list[4], (N_LAYER, PLANE), jnp.float32) ** levels(key_list[4], (N_LAYER, PLANE), ((0, 4), (1, 8)), -0.2, 0.2)), 0.25, 0.69921875).astype(jnp.bfloat16),
        "ranks": touch_ends(jax.random.randint(key_list[5], (N_LAYER, 6), RANK // 2, RANK + 1), jax.random.fold_in(key_list[5], 1), RANK // 2, RANK).astype(jnp.int32),
    }


def complex_rows(first, second, form):
    real_part = jnp.einsum(form, first[0], second[0]) - jnp.einsum(form, first[1], second[1])
    imag_part = jnp.einsum(form, first[0], second[1]) + jnp.einsum(form, first[1], second[0])
    return jnp.stack([real_part, imag_part])


def near_term(field, blocks):
    lower_side = jnp.pad(field[:, :, :-1], ((0, 0), (0, 0), (1, 0), (0, 0)))
    upper_side = jnp.pad(field[:, :, 1:], ((0, 0), (0, 0), (0, 1), (0, 0)))
    form = "rnp,nqp->rnq"
    total = complex_rows(field, blocks[0], form)
    total = total + complex_rows(lower_side, blocks[1], form)
    return total + complex_rows(upper_side, blocks[2], form)


def far_term(field, right_layer, left_layer, rank_row):
    total = jnp.zeros((2, RHS, PLANE), jnp.float32)
    for level, count in ((0, 2), (1, 4)):
        width = PLANE // count
        pieces = field.reshape(2, RHS, count, width)
        right_split = right_layer[level].reshape(2, RANK, count, width)
        coeff = complex_rows(pieces, right_split, "rcp,acp->rca")
        coeff = lax.optimization_barrier(coeff.astype(jnp.bfloat16)).astype(jnp.float32)
        swapped = coeff.reshape(2, RHS, count // 2, 2, RANK)[:, :, :, ::-1].reshape(2, RHS, count, RANK)
        limits = rank_row[2 * level:2 * level + count]
        keep = (jnp.arange(RANK)[None, :] < limits[:, None]).astype(jnp.float32)
        swapped = swapped * keep[None, None]
        left_split = left_layer[level].reshape(2, RANK, count, width)
        total = total + complex_rows(swapped, left_split, "rca,acp->rcp").reshape(2, RHS, PLANE)
    return total


def apply_inverse(layer_id, field_low, near_blocks, right_bases, left_bases, ranks):
    leaf_total = PLANE // CELLS
    field = field_low.astype(jnp.float32)
    blocks = near_blocks[layer_id].astype(jnp.float32).reshape(3, 2, leaf_total, CELLS, CELLS)
    near_value = near_term(field.reshape(2, RHS, leaf_total, CELLS), blocks).reshape(2, RHS, PLANE)
    far_value = far_term(field, right_bases[layer_id].astype(jnp.float32), left_bases[layer_id].astype(jnp.float32), ranks[layer_id])
    return near_value + far_value


def reference(right_side, near_blocks, right_bases, left_bases, coupling, ranks):
    def solve(layer_id, field_low):
        return apply_inverse(layer_id, field_low, near_blocks, right_bases, left_bases, ranks)

    inner = [solve(layer_id, right_side[layer_id]) for layer_id in range(N_LAYER)]
    forward = [inner[0].astype(jnp.bfloat16)]
    for layer_id in range(1, N_LAYER):
        coupled = (coupling[layer_id - 1].astype(jnp.float32) * forward[layer_id - 1].astype(jnp.float32)).astype(jnp.bfloat16)
        forward.append((inner[layer_id] - solve(layer_id, coupled)).astype(jnp.bfloat16))
    return jnp.stack(forward)
```

```python
import functools

import jax
import jax.numpy as jnp
from jax import lax
from jax.experimental import pallas as pl
from jax.experimental.pallas import tpu as pltpu
from jax.sharding import PartitionSpec as P

BATCHES = 2
SUM_TYPE = jnp.bfloat16
F32 = jnp.float32
BF16 = jnp.bfloat16
LANES = (((1,), (1,)), ((), ()))


def kernel(
    layers, leafs, batches,
    source_hbm, near_hbm, right_hbm, left_hbm, coupling_hbm, ranks_hbm,
    out_ref,
    source, near, near_turned, right, right_next, left_raw, left, coupling_ref, ranks_ref, inner, found,
    rim, part, part_sent, moved, sent, moved_rim, moved_part, moved_part_sent,
    load_sem, near_sem, rim_sem, part_sem, right_sem, move_sem, move_rim_sem, move_part_sem,
):
    layer = lax.axis_index("layer")
    leaf = lax.axis_index("leaf")
    rows, width = source.shape[1], source.shape[2]
    cells = near.shape[-1]
    count = width // cells
    rank = right.shape[2]
    group = rows // batches
    half, quarter = leafs // 2, leafs // 4
    upper, lower = leaf // half, leaf // quarter
    has_low, has_high = leaf > 0, leaf < leafs - 1
    odd, even = lax.rem(leaf, 2) == 1, lax.rem(leaf, 2) == 0
    has_prev, has_next = layer > 0, layer < layers - 1

    def remote(src, dst, sems, index, to_layer, to_leaf, landing=None):
        return pltpu.make_async_remote_copy(
            src_ref=src, dst_ref=dst,
            send_sem=sems.at[(0,) + index],
            recv_sem=sems.at[(1,) + (index if landing is None else landing)],
            device_id=(to_layer, to_leaf), device_id_type=pl.DeviceIdType.MESH,
        )

    loads = [
        pltpu.make_async_copy(source_hbm.at[0], source, load_sem.at[0]),
        pltpu.make_async_copy(right_hbm.at[0], right, load_sem.at[1]),
        pltpu.make_async_copy(left_hbm.at[0], left_raw, load_sem.at[2]),
        pltpu.make_async_copy(coupling_hbm, coupling_ref, load_sem.at[3]),
        pltpu.make_async_copy(ranks_hbm, ranks_ref, load_sem.at[4]),
    ]
    near_loads = [
        pltpu.make_async_copy(
            near_hbm.at[0, :, :, pl.ds(q * cells, cells), :], near.at[q], near_sem.at[q]
        )
        for q in range(count)
    ]
    order = list(range(1, count - 1)) + ([0, count - 1] if count > 1 else [0])
    barrier = pltpu.get_barrier_semaphore()

    def greet(to_layer, to_leaf):
        pl.semaphore_signal(
            barrier, inc=1, device_id=(to_layer, to_leaf), device_id_type=pl.DeviceIdType.MESH
        )

    for step in range(1, leafs):
        greet(layer, lax.rem(leaf + step, leafs))

    @pl.when(has_prev)
    def _():
        for other in range(leafs):
            greet(layer - 1, other)

    @pl.when(has_next)
    def _():
        for other in range(leafs):
            greet(layer + 1, other)

    for copy in loads:
        copy.start()
    for q in order:
        near_loads[q].start()

    @pl.when(jnp.logical_not(has_low))
    def _():
        rim[0] = jnp.zeros(rim.shape[1:], BF16)
        for b in range(batches):
            moved_rim[b, 0] = jnp.zeros(moved_rim.shape[2:], BF16)

    @pl.when(jnp.logical_not(has_high))
    def _():
        rim[1] = jnp.zeros(rim.shape[1:], BF16)
        for b in range(batches):
            moved_rim[b, 1] = jnp.zeros(moved_rim.shape[2:], BF16)

    def stacked(real, imag):
        return jnp.concatenate([real, imag], axis=0), jnp.concatenate([-imag, real], axis=0)

    def partial_sums(first, second, bases):
        flat = jnp.concatenate(
            [bases[:, 0].reshape(2 * rank, width), bases[:, 1].reshape(2 * rank, width)], axis=1
        )
        both = jnp.concatenate([first, second], axis=1)
        return lax.dot_general(flat, both, LANES, preferred_element_type=F32)

    def part_copies(src, dst, sems, index, to_layer):
        copies = []
        slot = lax.rem(leaf, half)
        for other in range(half):
            copies.append(remote(
                src.at[0], dst.at[slot], sems, index + (other,),
                to_layer, (1 - upper) * half + other, index + (slot,),
            ))
        slot = half + lax.rem(leaf, quarter)
        sibling = lower + 1 - 2 * lax.rem(lower, 2)
        for other in range(quarter):
            copies.append(remote(
                src.at[1], dst.at[slot], sems, index + (half + other,),
                to_layer, sibling * quarter + other, index + (slot,),
            ))
        return copies

    def part_arrivals(src, dst, sems, index):
        for slot in range(half + quarter):
            pltpu.make_async_copy(
                dst.at[slot], dst.at[slot], sems.at[(1,) + index + (slot,)]
            ).wait()

    def near_leaf(q, field, low, high, turned=False):
        pieces = []
        for at in (q, q - 1, q + 1):
            if at < 0:
                view = low
            elif at >= count:
                view = high
            else:
                view = field.at[:, :, pl.ds(at * cells, cells)]
            pieces.append(stacked(view[0], view[1]))
        lhs = jnp.concatenate([a for a, _ in pieces] + [b for _, b in pieces], axis=1)
        if turned:
            return jnp.dot(lhs, near_turned[q], preferred_element_type=F32)
        rhs = jnp.concatenate(
            [near[q, s, 0] for s in range(3)] + [near[q, s, 1] for s in range(3)], axis=1
        )
        return lax.dot_general(lhs, rhs, LANES, preferred_element_type=F32)

    def coefficients(parts):
        first = parts[0].astype(F32)
        for slot in range(1, half):
            first = first + parts[slot].astype(F32)
        second = parts[half].astype(F32)
        for slot in range(1, quarter):
            second = second + parts[half + slot].astype(F32)
        turned = jnp.concatenate([first, second], axis=0).T
        size = turned.shape[0] // 2
        swapped = jnp.concatenate([-turned[size:], turned[:size]], axis=0)
        return jnp.concatenate([turned, swapped], axis=1).astype(BF16)

    def far_leaf(q, coeff):
        span = pl.ds(q * cells, cells)
        return jnp.dot(coeff, left[:, span], preferred_element_type=F32)

    loads[0].wait()
    loads[1].wait()
    first, second = stacked(source[0], source[1])
    sums = partial_sums(first, second, right[...])
    for level in range(2):
        part_sent[level] = sums[level * rank:(level + 1) * rank].astype(SUM_TYPE)

    pl.semaphore_wait(
        barrier,
        leafs - 1 + leafs * has_prev.astype(jnp.int32) + leafs * has_next.astype(jnp.int32),
    )

    to_high = remote(
        source.at[:, :, pl.ds(width - cells, cells)], rim.at[0], rim_sem, (0,), layer, leaf + 1
    )
    to_low = remote(source.at[:, :, pl.ds(0, cells)], rim.at[1], rim_sem, (1,), layer, leaf - 1)
    source_parts = part_copies(part_sent, part, part_sem, (), layer)
    down = remote(right, right_next, right_sem, (), layer - 1, leaf)
    pl.when(has_high)(to_high.start)
    pl.when(has_low)(to_low.start)
    for copy in source_parts:
        copy.start()
    pl.when(has_prev)(down.start)

    loads[2].wait()
    loads[3].wait()
    loads[4].wait()
    row_ids = lax.broadcasted_iota(jnp.int32, (rank, width), 0)
    for level, slot in ((0, upper), (1, 2 + lower)):
        keep = (row_ids < ranks_ref[0, slot]).astype(F32)
        for c in range(2):
            left[pl.ds((2 * c + level) * rank, rank), :] = (
                left_raw[level, c].astype(F32) * keep
            ).astype(BF16)

    for q in order:
        if q == order[max(count - 2, 0)]:
            pl.when(has_low)(to_high.wait_recv)
            pl.when(has_high)(to_low.wait_recv)
        near_loads[q].wait()
        inner[:, :, pl.ds(q * cells, cells)] = near_leaf(
            q, source, rim.at[0], rim.at[1]
        ).reshape(2, rows, cells)
    part_arrivals(part_sent, part, part_sem, ())
    coeff = coefficients(part)
    for q in range(count):
        span = pl.ds(q * cells, cells)
        inner[:, :, span] += far_leaf(q, coeff).reshape(2, rows, cells)

    @pl.when(has_prev)
    def _():
        for q in range(count):
            for c in range(2):
                for s in range(3):
                    near_turned[q, pl.ds((3 * c + s) * cells, cells), :] = near[q, s, c].T

    in_flight = []
    for b in range(batches):
        span_rows = pl.ds(b * group, group)
        spans = [(0, width)]
        ahead = [
            remote(
                sent.at[b, :, :, pl.ds(*span)], moved.at[b, :, :, pl.ds(*span)],
                move_sem, (b, piece), layer + 1, leaf,
            )
            for piece, span in enumerate(spans)
        ]
        across_high = remote(
            moved.at[b, :, :, pl.ds(width - cells, cells)], moved_rim.at[b, 0],
            move_rim_sem, (b, 0), layer, leaf + 1,
        )
        across_low = remote(
            moved.at[b, :, :, pl.ds(0, cells)], moved_rim.at[b, 1],
            move_rim_sem, (b, 1), layer, leaf - 1,
        )
        ahead_high = remote(
            sent.at[b, :, :, pl.ds(width - cells, cells)], moved_rim.at[b, 0],
            move_rim_sem, (b, 0), layer + 1, leaf + 1,
        )
        ahead_low = remote(
            sent.at[b, :, :, pl.ds(0, cells)], moved_rim.at[b, 1],
            move_rim_sem, (b, 1), layer + 1, leaf - 1,
        )
        ahead_parts = part_copies(
            moved_part_sent.at[b], moved_part.at[b], move_part_sem, (b,), layer + 1
        )

        in_flight.append(
            (ahead, ahead_parts, across_low, across_high, ahead_high, ahead_low)
        )

        @pl.when(jnp.logical_not(has_prev))
        def _():
            out_ref[0, :, span_rows, :] = inner[:, span_rows, :].astype(BF16)

        @pl.when(has_prev)
        def _():
            ahead[0].wait_recv()
            pl.when(odd)(across_low.start)
            pl.when(even)(across_high.start)
            for q in order:
                if q == order[max(count - 2, 0)]:
                    pl.when(has_low)(ahead_high.wait_recv)
                    pl.when(has_high)(ahead_low.wait_recv)
                found[q] = near_leaf(q, moved.at[b], moved_rim.at[b, 0], moved_rim.at[b, 1], True)
            part_arrivals(moved_part_sent.at[b], moved_part.at[b], move_part_sem, (b,))
            coeff = coefficients(moved_part[b])
            for q in range(count):
                span = pl.ds(q * cells, cells)
                update = (found[q] + far_leaf(q, coeff)).reshape(2, group, cells)
                out_ref[0, :, span_rows, span] = (
                    inner[:, span_rows, span] - update
                ).astype(BF16)

        @pl.when(has_next)
        def _():
            swept = out_ref[0, :, span_rows, :].astype(F32)
            coupled = (coupling_ref[...].astype(F32)[None] * swept).astype(BF16)
            sent[b] = coupled
            ahead[0].start()
            first, second = stacked(coupled[0], coupled[1])
            if b == 0:
                down.wait_recv()
            sums = partial_sums(first, second, right_next[...])
            for level in range(2):
                moved_part_sent[b, level] = sums[level * rank:(level + 1) * rank].astype(SUM_TYPE)
            for copy in ahead_parts:
                copy.start()
            pl.when(odd & has_high)(ahead_high.start)
            pl.when(even & has_low)(ahead_low.start)

    pl.when(has_high)(to_high.wait_send)
    pl.when(has_low)(to_low.wait_send)
    for copy in source_parts:
        copy.wait_send()
    pl.when(has_prev)(down.wait_send)

    for b in range(batches):
        flights = in_flight[b]

        @pl.when(has_prev)
        def _():
            pl.when(odd)(flights[2].wait_send)
            pl.when(even)(flights[3].wait_send)

        @pl.when(has_next)
        def _():
            for copy in flights[0] + flights[1]:
                copy.wait_send()
            pl.when(odd & has_high)(flights[4].wait_send)
            pl.when(even & has_low)(flights[5].wait_send)


def body(layers, leafs, right_side, near_blocks, right_bases, left_bases, coupling, ranks):
    rows, width = right_side.shape[2:]
    cells = near_blocks.shape[-1]
    rank = right_bases.shape[3]
    count = width // cells
    batches = BATCHES
    group = rows // batches
    sources = leafs // 2 + leafs // 4
    anywhere = pl.BlockSpec(memory_space=pl.ANY)
    vmem = pl.BlockSpec(memory_space=pltpu.VMEM)
    dma = pltpu.SemaphoreType.DMA
    return pl.pallas_call(
        functools.partial(kernel, layers, leafs, batches),
        out_shape=pltpu.VMEM(right_side.shape, BF16),
        in_specs=[anywhere] * 6,
        out_specs=vmem,
        scratch_shapes=[
            pltpu.VMEM((2, rows, width), BF16),
            pltpu.VMEM((count, 3, 2, cells, cells), BF16),
            pltpu.VMEM((count, 6 * cells, cells), BF16),
            pltpu.VMEM((2, 2, rank, width), BF16),
            pltpu.VMEM((2, 2, rank, width), BF16),
            pltpu.VMEM((2, 2, rank, width), BF16),
            pltpu.VMEM((4 * rank, width), BF16),
            pltpu.VMEM(coupling.shape, BF16),
            pltpu.SMEM(ranks.shape, jnp.int32),
            pltpu.VMEM((2, rows, width), F32),
            pltpu.VMEM((count, 2 * group, cells), F32),
            pltpu.VMEM((2, 2, rows, cells), BF16),
            pltpu.VMEM((sources, rank, 2 * rows), SUM_TYPE),
            pltpu.VMEM((2, rank, 2 * rows), SUM_TYPE),
            pltpu.VMEM((batches, 2, group, width), BF16),
            pltpu.VMEM((batches, 2, group, width), BF16),
            pltpu.VMEM((batches, 2, 2, group, cells), BF16),
            pltpu.VMEM((batches, sources, rank, 2 * group), SUM_TYPE),
            pltpu.VMEM((batches, 2, rank, 2 * group), SUM_TYPE),
            dma((5,)),
            dma((count,)),
            dma((2, 2)),
            dma((2, sources)),
            dma((2,)),
            dma((2, batches, 1)),
            dma((2, batches, 2)),
            dma((2, batches, sources)),
        ],
        compiler_params=pltpu.CompilerParams(collective_id=0, has_side_effects=True),
    )(right_side, near_blocks, right_bases, left_bases, coupling, ranks)


def solution(mesh):
    placed = (
        P("layer", None, None, "leaf"),
        P("layer", None, None, "leaf", None),
        P("layer", None, None, None, "leaf"),
        P("layer", None, None, None, "leaf"),
        P("layer", "leaf"),
        P("layer", None),
    )
    return jax.shard_map(
        functools.partial(body, mesh.shape["layer"], mesh.shape["leaf"]),
        mesh=mesh, in_specs=placed, out_specs=P("layer", None, None, "leaf"), check_vma=False,
    )
```

```python
import functools

import jax
import jax.numpy as jnp
from jax import lax
from jax.experimental import pallas as pl
from jax.experimental.pallas import tpu as pltpu
from jax.sharding import PartitionSpec as P

BATCHES = 2
FOLD = 8
F32 = jnp.float32
BF16 = jnp.bfloat16
LANES = (((1,), (1,)), ((), ()))


def kernel(
    layers, leafs, batches,
    source_hbm, near_hbm, right_hbm, left_hbm, coupling_hbm, ranks_hbm,
    out_ref,
    source, near, near_turned, right, right_next, left_raw, left, coupling_ref, ranks_ref,
    inner, base, rim, part, part_sent, moved, sent, moved_rim, moved_part, moved_part_sent,
    load_sem, near_sem, rim_sem, part_sem, right_sem, move_sem, move_rim_sem, move_part_sem, sent_sem,
):
    layer = lax.axis_index("layer")
    leaf = lax.axis_index("leaf")
    rows, width = source.shape[1], source.shape[2]
    cells = near.shape[-1]
    count = width // cells
    rank = right.shape[2]
    group = rows // batches
    half, quarter = leafs // 2, leafs // 4
    upper, lower = leaf // half, leaf // quarter
    has_low, has_high = leaf > 0, leaf < leafs - 1
    has_prev, has_next = layer > 0, layer < layers - 1
    edges = [0, count - 1] if count > 1 else [0]

    def remote(src, dst, sems, index, to_layer, to_leaf):
        return pltpu.make_async_remote_copy(
            src_ref=src, dst_ref=dst,
            send_sem=sems.at[(0,) + index],
            recv_sem=sems.at[(1,) + index],
            device_id=(to_layer, to_leaf), device_id_type=pl.DeviceIdType.MESH,
        )

    barrier = pltpu.get_barrier_semaphore()

    def greet(to_layer, to_leaf):
        pl.semaphore_signal(
            barrier, inc=1, device_id=(to_layer, to_leaf), device_id_type=pl.DeviceIdType.MESH
        )

    for step in range(1, leafs):
        greet(layer, lax.rem(leaf + step, leafs))

    @pl.when(has_prev)
    def _():
        for other in range(leafs):
            greet(layer - 1, other)

    @pl.when(has_next)
    def _():
        for other in range(leafs):
            greet(layer + 1, other)

    loads = [
        pltpu.make_async_copy(source_hbm.at[0], source, load_sem.at[0]),
        pltpu.make_async_copy(right_hbm.at[0], right, load_sem.at[1]),
        pltpu.make_async_copy(left_hbm.at[0], left_raw, load_sem.at[2]),
        pltpu.make_async_copy(coupling_hbm, coupling_ref, load_sem.at[3]),
        pltpu.make_async_copy(ranks_hbm, ranks_ref, load_sem.at[4]),
    ]
    near_loads = [
        pltpu.make_async_copy(
            near_hbm.at[0, :, :, pl.ds(q * cells, cells), :], near.at[q], near_sem.at[q]
        )
        for q in range(count)
    ]
    for copy in loads + near_loads:
        copy.start()

    @pl.when(jnp.logical_not(has_low))
    def _():
        rim[0] = jnp.zeros(rim.shape[1:], BF16)
        for b in range(batches):
            moved_rim[b, 0] = jnp.zeros(moved_rim.shape[2:], BF16)

    @pl.when(jnp.logical_not(has_high))
    def _():
        rim[1] = jnp.zeros(rim.shape[1:], BF16)
        for b in range(batches):
            moved_rim[b, 1] = jnp.zeros(moved_rim.shape[2:], BF16)

    def block(q):
        return pl.ds(q * cells, cells)

    def stacked(real, imag):
        return jnp.concatenate(
            [
                jnp.concatenate([real, imag], axis=0),
                jnp.concatenate([-imag, real], axis=0),
            ],
            axis=1,
        )

    def piece(field, q):
        return stacked(field[0, :, block(q)], field[1, :, block(q)])

    def sides(q):
        return [0] + ([1] if q > 0 else []) + ([2] if q < count - 1 else [])

    def shifted(q, s):
        return q + (0, -1, 1)[s]

    def folded(pieces, bases):
        total = None
        for q in range(count):
            flat = jnp.concatenate(
                [bases[:, c, :, block(q)].reshape(2 * rank, cells) for c in range(2)], axis=1
            )
            term = lax.dot_general(pieces[q], flat, LANES, preferred_element_type=F32)
            total = term if total is None else total + term
        return jnp.concatenate(
            [total[at:at + FOLD] for at in range(0, total.shape[0], FOLD)], axis=1
        ).astype(BF16)

    def part_copies(src, dst, sems, index, to_layer):
        copies = []
        slot = lax.rem(leaf, half)
        for other in range(half):
            copies.append(remote(
                src, dst.at[slot], sems, index,
                to_layer, (1 - upper) * half + other,
            ))
        slot = half + lax.rem(leaf, quarter)
        sibling = lower + 1 - 2 * lax.rem(lower, 2)
        for other in range(quarter):
            copies.append(remote(
                src, dst.at[slot], sems, index,
                to_layer, sibling * quarter + other,
            ))
        return copies

    def part_waits(dst, sems, index, way):
        pltpu.make_async_copy(dst, dst, sems.at[(way,) + index]).wait()

    def coefficients(parts):
        first = parts[0].astype(F32)
        for slot in range(1, half):
            first = first + parts[slot].astype(F32)
        second = parts[half].astype(F32)
        for slot in range(1, quarter):
            second = second + parts[half + slot].astype(F32)
        column = lax.broadcasted_iota(jnp.int32, first.shape, 1)
        both = jnp.where(lax.rem(column, 2 * rank) < rank, first, second)
        turned = jnp.concatenate(
            [both[:, at:at + 2 * rank] for at in range(0, both.shape[1], 2 * rank)], axis=0
        )
        size = turned.shape[0] // 2
        swapped = jnp.concatenate([-turned[size:], turned[:size]], axis=0)
        return jnp.concatenate([turned, swapped], axis=1).astype(BF16)

    def far_leaf(q, coeff):
        return jnp.dot(coeff, left[:, block(q)], preferred_element_type=F32)

    def plain_dot(q, s, value):
        rhs = jnp.concatenate([near[q, s, 0], near[q, s, 1]], axis=1)
        return lax.dot_general(value, rhs, LANES, preferred_element_type=F32)

    def turned_dot(q, chosen, values):
        rhs = [near_turned[q, pl.ds(s * 2 * cells, 2 * cells), :] for s in chosen]
        return jnp.dot(
            jnp.concatenate(values, axis=1), jnp.concatenate(rhs, axis=0),
            preferred_element_type=F32,
        )

    loads[0].wait()
    loads[1].wait()
    source_pieces = [piece(source, q) for q in range(count)]
    part_sent[...] = folded(source_pieces, right)

    pl.semaphore_wait(
        barrier,
        leafs - 1 + leafs * has_prev.astype(jnp.int32) + leafs * has_next.astype(jnp.int32),
    )

    to_high = remote(
        source.at[:, :, block(count - 1)], rim.at[0], rim_sem, (0,), layer, leaf + 1
    )
    to_low = remote(source.at[:, :, block(0)], rim.at[1], rim_sem, (1,), layer, leaf - 1)
    source_parts = part_copies(part_sent, part, part_sem, (), layer)
    down = remote(right, right_next, right_sem, (), layer - 1, leaf)
    for copy in source_parts:
        copy.start()
    pl.when(has_high)(to_high.start)
    pl.when(has_low)(to_low.start)
    pl.when(has_prev)(down.start)

    loads[2].wait()
    loads[3].wait()
    loads[4].wait()
    row_ids = lax.broadcasted_iota(jnp.int32, (rank, width), 0)
    for level, slot in ((0, upper), (1, 2 + lower)):
        keep = (row_ids < ranks_ref[0, slot]).astype(F32)
        for c in range(2):
            left[pl.ds((2 * c + level) * rank, rank), :] = (
                left_raw[level, c].astype(F32) * keep
            ).astype(BF16)

    for q in range(count):
        near_loads[q].wait()
        value = None
        for s in sides(q):
            term = plain_dot(q, s, source_pieces[shifted(q, s)])
            value = term if value is None else value + term
        inner[:, :, block(q)] = value.reshape(2, rows, cells)
    pl.when(has_low)(to_high.wait_recv)
    pl.when(has_high)(to_low.wait_recv)
    for q, s, side in ((0, 1, 0), (count - 1, 2, 1)):
        inner[:, :, block(q)] += plain_dot(q, s, stacked(rim[side, 0], rim[side, 1])).reshape(
            2, rows, cells
        )
    part_waits(part, part_sem, (), 1)
    coeff = coefficients(part)
    for q in range(count):
        inner[:, :, block(q)] += far_leaf(q, coeff).reshape(2, rows, cells)

    @pl.when(has_prev)
    def _():
        for q in range(count):
            for s in range(3):
                for c in range(2):
                    near_turned[q, pl.ds((2 * s + c) * cells, cells), :] = near[q, s, c].T

    def rows_of(b):
        return pl.ds(b * group, group)

    def ahead_main(b):
        pairs = [(block(q), 0) for q in edges]
        if count > 2:
            pairs.append((pl.ds(cells, width - 2 * cells), 1))
        return [
            pltpu.make_async_remote_copy(
                src_ref=sent.at[b, :, :, span], dst_ref=moved.at[b, :, :, span],
                send_sem=sent_sem.at[0], recv_sem=move_sem.at[b, kind],
                device_id=(layer + 1, leaf), device_id_type=pl.DeviceIdType.MESH,
            )
            for span, kind in pairs
        ]

    def rim_copy(source_ref, q, b, side, to_layer, to_leaf):
        return pltpu.make_async_remote_copy(
            src_ref=source_ref.at[b, :, :, block(q)], dst_ref=moved_rim.at[b, side],
            send_sem=sent_sem.at[1 + side], recv_sem=move_rim_sem.at[b, side],
            device_id=(to_layer, to_leaf), device_id_type=pl.DeviceIdType.MESH,
        )

    def ahead_high(b):
        return rim_copy(sent, count - 1, b, 0, layer + 1, leaf + 1)

    def ahead_low(b):
        return rim_copy(sent, 0, b, 1, layer + 1, leaf - 1)

    def ahead_parts(b):
        return part_copies(
            moved_part_sent.at[b], moved_part.at[b], move_part_sem, (b,), layer + 1
        )

    def receive(b):
        view = moved.at[b, :, :, pl.ds(0, len(edges) * cells)]
        pltpu.make_async_copy(view, view, move_sem.at[b, 0]).wait()
        if count > 2:
            view = moved.at[b, :, :, pl.ds(cells, width - 2 * cells)]
            pltpu.make_async_copy(view, view, move_sem.at[b, 1]).wait()
        pl.when(has_low)(ahead_high(b).wait_recv)
        pl.when(has_high)(ahead_low(b).wait_recv)
        pieces = [stacked(moved_rim[b, 0, 0], moved_rim[b, 0, 1])]
        pieces += [piece(moved.at[b], q) for q in range(count)]
        pieces += [stacked(moved_rim[b, 1, 0], moved_rim[b, 1, 1])]
        for q in range(count):
            base[q] = inner[:, rows_of(b), block(q)].reshape(2 * group, cells) - turned_dot(
                q, range(3), [pieces[q + 1], pieces[q], pieces[q + 2]]
            )
        part_waits(moved_part.at[b], move_part_sem, (b,), 1)
        coeff = coefficients(moved_part[b])
        fields = []
        for q in range(count):
            swept = (base[q] - far_leaf(q, coeff)).astype(BF16).reshape(2, group, cells)
            out_ref[0, :, rows_of(b), block(q)] = swept
            fields.append(swept)
        return fields

    def emit(b, fields, first):
        coupled = []
        for q in range(count):
            value = (coupling_ref[:, block(q)].astype(F32)[None] * fields[q].astype(F32)).astype(BF16)
            sent[b, :, :, block(q)] = value
            coupled.append(value)
        pl.when(has_high)(ahead_high(b).start)
        pl.when(has_low)(ahead_low(b).start)
        if first and b == 0:
            for copy in ahead_main(b):
                copy.start()
        if b == 0:
            down.wait_recv()
        moved_part_sent[b] = folded([stacked(v[0], v[1]) for v in coupled], right_next)
        for copy in ahead_parts(b):
            copy.start()
        if not (first and b == 0):
            for copy in ahead_main(b):
                copy.start()

    @pl.when(jnp.logical_not(has_prev))
    def _():
        for b in range(batches):
            out_ref[0, :, rows_of(b), :] = inner[:, rows_of(b), :].astype(BF16)

            @pl.when(has_next)
            def _():
                emit(b, [out_ref[0, :, rows_of(b), block(q)] for q in range(count)], True)

    @pl.when(has_prev & has_next)
    def _():
        for b in range(batches):
            emit(b, receive(b), False)

    @pl.when(has_prev & jnp.logical_not(has_next))
    def _():
        for b in range(batches):
            receive(b)

    pl.when(has_high)(to_high.wait_send)
    pl.when(has_low)(to_low.wait_send)
    part_waits(part, part_sem, (), 0)
    pl.when(has_prev)(down.wait_send)

    def drained(ref, index):
        pltpu.make_async_copy(ref, ref, sent_sem.at[index]).wait()

    @pl.when(has_next)
    def _():
        drained(sent, 0)
        pl.when(has_high)(lambda: drained(moved_rim.at[:, 0], 1))
        pl.when(has_low)(lambda: drained(moved_rim.at[:, 1], 2))
        for b in range(batches):
            part_waits(moved_part.at[b], move_part_sem, (b,), 0)


def body(layers, leafs, right_side, near_blocks, right_bases, left_bases, coupling, ranks):
    rows, width = right_side.shape[2:]
    cells = near_blocks.shape[-1]
    rank = right_bases.shape[3]
    count = width // cells
    batches = BATCHES
    group = rows // batches
    sources = leafs // 2 + leafs // 4
    dma = pltpu.SemaphoreType.DMA

    def fold_shape(size):
        return (FOLD, 2 * size // FOLD * 2 * rank)

    return pl.pallas_call(
        functools.partial(kernel, layers, leafs, batches),
        out_shape=pltpu.VMEM(right_side.shape, BF16),
        in_specs=[pl.BlockSpec(memory_space=pl.ANY)] * 6,
        out_specs=pl.BlockSpec(memory_space=pltpu.VMEM),
        scratch_shapes=[
            pltpu.VMEM((2, rows, width), BF16),
            pltpu.VMEM((count, 3, 2, cells, cells), BF16),
            pltpu.VMEM((count, 6 * cells, cells), BF16),
            pltpu.VMEM((2, 2, rank, width), BF16),
            pltpu.VMEM((2, 2, rank, width), BF16),
            pltpu.VMEM((2, 2, rank, width), BF16),
            pltpu.VMEM((4 * rank, width), BF16),
            pltpu.VMEM(coupling.shape, BF16),
            pltpu.SMEM(ranks.shape, jnp.int32),
            pltpu.VMEM((2, rows, width), F32),
            pltpu.VMEM((count, 2 * group, cells), F32),
            pltpu.VMEM((2, 2, rows, cells), BF16),
            pltpu.VMEM((sources,) + fold_shape(rows), BF16),
            pltpu.VMEM(fold_shape(rows), BF16),
            pltpu.VMEM((batches, 2, group, width), BF16),
            pltpu.VMEM((batches, 2, group, width), BF16),
            pltpu.VMEM((batches, 2, 2, group, cells), BF16),
            pltpu.VMEM((batches, sources) + fold_shape(group), BF16),
            pltpu.VMEM((batches,) + fold_shape(group), BF16),
            dma((5,)),
            dma((count,)),
            dma((2, 2)),
            dma((2,)),
            dma((2,)),
            dma((batches, 2)),
            dma((batches, 2)),
            dma((2, batches)),
            dma((3,)),
        ],
        compiler_params=pltpu.CompilerParams(collective_id=0, has_side_effects=True),
    )(right_side, near_blocks, right_bases, left_bases, coupling, ranks)


def solution(mesh):
    placed = (
        P("layer", None, None, "leaf"),
        P("layer", None, None, "leaf", None),
        P("layer", None, None, None, "leaf"),
        P("layer", None, None, None, "leaf"),
        P("layer", "leaf"),
        P("layer", None),
    )
    return jax.shard_map(
        functools.partial(body, mesh.shape["layer"], mesh.shape["leaf"]),
        mesh=mesh, in_specs=placed, out_specs=P("layer", None, None, "leaf"), check_vma=False,
    )
```

```python
import functools

import jax
import jax.numpy as jnp
from jax import lax
from jax.experimental import pallas as pl
from jax.experimental.pallas import tpu as pltpu
from jax.sharding import PartitionSpec as P

BATCHES = 4
TILE = 128
F32 = jnp.float32
BF16 = jnp.bfloat16
LANES = (((1,), (1,)), ((), ()))


def kernel(
    layers, leafs, batches,
    source_hbm, near_hbm, right_hbm, left_hbm, coupling_hbm, ranks_hbm,
    out_ref,
    source, near, near_turned, right, right_next, left_raw, left, coupling_ref, ranks_ref,
    inner, base, rim, part, part_sent, moved, sent, moved_rim, moved_part, moved_part_sent,
    load_sem, near_sem, rim_sem, part_sem, right_sem, move_sem, move_rim_sem, move_part_sem, sent_sem, ready_sem,
):
    layer = lax.axis_index("layer")
    leaf = lax.axis_index("leaf")
    rows, width = source.shape[1], source.shape[2]
    cells = near.shape[-1]
    count = width // cells
    rank = right.shape[2]
    group = rows // batches
    half, quarter = leafs // 2, leafs // 4
    upper, lower = leaf // half, leaf // quarter
    has_low, has_high = leaf > 0, leaf < leafs - 1
    has_prev, has_next = layer > 0, layer < layers - 1
    edges = [0, count - 1] if count > 1 else [0]

    def remote(src, dst, sems, index, to_layer, to_leaf):
        return pltpu.make_async_remote_copy(
            src_ref=src, dst_ref=dst,
            send_sem=sems.at[(0,) + index],
            recv_sem=sems.at[(1,) + index],
            device_id=(to_layer, to_leaf), device_id_type=pl.DeviceIdType.MESH,
        )

    barrier = pltpu.get_barrier_semaphore()

    def greet(to_layer, to_leaf):
        pl.semaphore_signal(
            barrier, inc=1, device_id=(to_layer, to_leaf), device_id_type=pl.DeviceIdType.MESH
        )

    for step in range(1, leafs):
        greet(layer, lax.rem(leaf + step, leafs))

    pl.when(has_prev)(lambda: greet(layer - 1, leaf))
    pl.when(has_next)(lambda: greet(layer + 1, leaf))

    loads = [
        pltpu.make_async_copy(source_hbm.at[0], source, load_sem.at[0]),
        pltpu.make_async_copy(right_hbm.at[0], right, load_sem.at[1]),
        pltpu.make_async_copy(left_hbm.at[0], left_raw, load_sem.at[2]),
        pltpu.make_async_copy(coupling_hbm, coupling_ref, load_sem.at[3]),
        pltpu.make_async_copy(ranks_hbm, ranks_ref, load_sem.at[4]),
    ]
    near_loads = [
        pltpu.make_async_copy(
            near_hbm.at[0, :, :, pl.ds(q * cells, cells), :], near.at[q], near_sem.at[q]
        )
        for q in range(count)
    ]
    for copy in loads + near_loads:
        copy.start()

    @pl.when(jnp.logical_not(has_low))
    def _():
        rim[0] = jnp.zeros(rim.shape[1:], BF16)
        for b in range(batches):
            moved_rim[b, 0] = jnp.zeros(moved_rim.shape[2:], BF16)

    @pl.when(jnp.logical_not(has_high))
    def _():
        rim[1] = jnp.zeros(rim.shape[1:], BF16)
        for b in range(batches):
            moved_rim[b, 1] = jnp.zeros(moved_rim.shape[2:], BF16)

    def block(q):
        return pl.ds(q * cells, cells)

    def stacked(real, imag):
        return jnp.concatenate(
            [
                jnp.concatenate([real, imag], axis=0),
                jnp.concatenate([-imag, real], axis=0),
            ],
            axis=1,
        )

    def piece(field, q):
        return stacked(field[0, :, block(q)], field[1, :, block(q)])

    def sides(q):
        return [0] + ([1] if q > 0 else []) + ([2] if q < count - 1 else [])

    def shifted(q, s):
        return q + (0, -1, 1)[s]

    def folded(pieces, bases):
        total = None
        for q in range(count):
            flat = jnp.concatenate(
                [bases[:, c, :, block(q)].reshape(2 * rank, cells) for c in range(2)], axis=1
            )
            term = lax.dot_general(pieces[q], flat, LANES, preferred_element_type=F32)
            total = term if total is None else total + term
        height = max(total.shape[0] * total.shape[1] // TILE, 1)
        return jnp.concatenate(
            [total[at:at + height] for at in range(0, total.shape[0], height)], axis=1
        ).astype(BF16)

    def part_copies(src, dst, sems, index, to_layer):
        copies = []
        slot = lax.rem(leaf, half)
        for other in range(half):
            copies.append(remote(
                src, dst.at[slot], sems, index,
                to_layer, (1 - upper) * half + other,
            ))
        slot = half + lax.rem(leaf, quarter)
        sibling = lower + 1 - 2 * lax.rem(lower, 2)
        for other in range(quarter):
            copies.append(remote(
                src, dst.at[slot], sems, index,
                to_layer, sibling * quarter + other,
            ))
        return copies

    def part_waits(dst, sems, index, way):
        pltpu.make_async_copy(dst, dst, sems.at[(way,) + index]).wait()

    def coefficients(parts):
        first = parts[0].astype(F32)
        for slot in range(1, half):
            first = first + parts[slot].astype(F32)
        second = parts[half].astype(F32)
        for slot in range(1, quarter):
            second = second + parts[half + slot].astype(F32)
        column = lax.broadcasted_iota(jnp.int32, first.shape, 1)
        both = jnp.where(lax.rem(column, 2 * rank) < rank, first, second)
        turned = jnp.concatenate(
            [both[:, at:at + 2 * rank] for at in range(0, both.shape[1], 2 * rank)], axis=0
        )
        size = turned.shape[0] // 2
        swapped = jnp.concatenate([-turned[size:], turned[:size]], axis=0)
        return jnp.concatenate([turned, swapped], axis=1).astype(BF16)

    def far_leaf(q, coeff):
        return jnp.dot(coeff, left[:, block(q)], preferred_element_type=F32)

    def plain_dot(q, s, value):
        rhs = jnp.concatenate([near[q, s, 0], near[q, s, 1]], axis=1)
        return lax.dot_general(value, rhs, LANES, preferred_element_type=F32)

    def turned_dot(q, chosen, values):
        rhs = [near_turned[q, pl.ds(s * 2 * cells, 2 * cells), :] for s in chosen]
        return jnp.dot(
            jnp.concatenate(values, axis=1), jnp.concatenate(rhs, axis=0),
            preferred_element_type=F32,
        )

    loads[0].wait()
    loads[1].wait()
    source_pieces = [piece(source, q) for q in range(count)]
    part_sent[...] = folded(source_pieces, right)

    pl.semaphore_wait(
        barrier, leafs - 1 + has_prev.astype(jnp.int32) + has_next.astype(jnp.int32)
    )

    to_high = remote(
        source.at[:, :, block(count - 1)], rim.at[0], rim_sem, (0,), layer, leaf + 1
    )
    to_low = remote(source.at[:, :, block(0)], rim.at[1], rim_sem, (1,), layer, leaf - 1)
    source_parts = part_copies(part_sent, part, part_sem, (), layer)

    @pl.when(has_prev)
    def _():
        pl.semaphore_signal(
            ready_sem, inc=1, device_id=(layer - 1, leaf), device_id_type=pl.DeviceIdType.MESH
        )

    down = remote(right, right_next, right_sem, (), layer - 1, leaf)
    for copy in source_parts:
        copy.start()
    pl.when(has_high)(to_high.start)
    pl.when(has_low)(to_low.start)
    pl.when(has_prev)(down.start)

    loads[2].wait()
    loads[3].wait()
    loads[4].wait()
    row_ids = lax.broadcasted_iota(jnp.int32, (rank, width), 0)
    for level, slot in ((0, upper), (1, 2 + lower)):
        keep = (row_ids < ranks_ref[0, slot]).astype(F32)
        for c in range(2):
            left[pl.ds((2 * c + level) * rank, rank), :] = (
                left_raw[level, c].astype(F32) * keep
            ).astype(BF16)

    for q in range(count):
        near_loads[q].wait()
        value = None
        for s in sides(q):
            term = plain_dot(q, s, source_pieces[shifted(q, s)])
            value = term if value is None else value + term
        inner[:, :, block(q)] = value.reshape(2, rows, cells)
    pl.when(has_low)(to_high.wait_recv)
    pl.when(has_high)(to_low.wait_recv)
    for q, s, side in ((0, 1, 0), (count - 1, 2, 1)):
        inner[:, :, block(q)] += plain_dot(q, s, stacked(rim[side, 0], rim[side, 1])).reshape(
            2, rows, cells
        )
    part_waits(part, part_sem, (), 1)
    coeff = coefficients(part)
    for q in range(count):
        inner[:, :, block(q)] += far_leaf(q, coeff).reshape(2, rows, cells)

    @pl.when(has_prev)
    def _():
        for q in range(count):
            for s in range(3):
                for c in range(2):
                    near_turned[q, pl.ds((2 * s + c) * cells, cells), :] = near[q, s, c].T

    pl.when(has_next)(lambda: pl.semaphore_wait(ready_sem, 1))

    def rows_of(b):
        return pl.ds(b * group, group)

    def ahead_main(b):
        pairs = [(block(q), 0) for q in edges]
        if count > 2:
            pairs.append((pl.ds(cells, width - 2 * cells), 1))
        return [
            pltpu.make_async_remote_copy(
                src_ref=sent.at[b, :, :, span], dst_ref=moved.at[b, :, :, span],
                send_sem=sent_sem.at[0], recv_sem=move_sem.at[b, kind],
                device_id=(layer + 1, leaf), device_id_type=pl.DeviceIdType.MESH,
            )
            for span, kind in pairs
        ]

    def rim_copy(source_ref, q, b, side, to_layer, to_leaf):
        return pltpu.make_async_remote_copy(
            src_ref=source_ref.at[b, :, :, block(q)], dst_ref=moved_rim.at[b, side],
            send_sem=sent_sem.at[1 + side], recv_sem=move_rim_sem.at[b, side],
            device_id=(to_layer, to_leaf), device_id_type=pl.DeviceIdType.MESH,
        )

    def ahead_high(b):
        return rim_copy(sent, count - 1, b, 0, layer + 1, leaf + 1)

    def ahead_low(b):
        return rim_copy(sent, 0, b, 1, layer + 1, leaf - 1)

    def ahead_parts(b):
        return part_copies(
            moved_part_sent.at[b], moved_part.at[b], move_part_sem, (b,), layer + 1
        )

    def wait_edges(b):
        view = moved.at[b, :, :, pl.ds(0, len(edges) * cells)]
        pltpu.make_async_copy(view, view, move_sem.at[b, 0]).wait()

    def wait_middle(b):
        if count > 2:
            view = moved.at[b, :, :, pl.ds(cells, width - 2 * cells)]
            pltpu.make_async_copy(view, view, move_sem.at[b, 1]).wait()

    def wait_rims(b):
        pl.when(has_low)(ahead_high(b).wait_recv)
        pl.when(has_high)(ahead_low(b).wait_recv)

    def receive_whole(b):
        wait_edges(b)
        wait_middle(b)
        wait_rims(b)
        part_waits(moved_part.at[b], move_part_sem, (b,), 1)
        coeff = coefficients(moved_part[b])
        pieces = [stacked(moved_rim[b, 0, 0], moved_rim[b, 0, 1])]
        pieces += [piece(moved.at[b], q) for q in range(count)]
        pieces += [stacked(moved_rim[b, 1, 0], moved_rim[b, 1, 1])]
        fields = []
        for q in range(count):
            lhs = jnp.concatenate([pieces[q + 1], pieces[q], pieces[q + 2], coeff], axis=1)
            rhs = jnp.concatenate([near_turned[q], left[:, block(q)]], axis=0)
            value = inner[:, rows_of(b), block(q)].reshape(2 * group, cells) - jnp.dot(
                lhs, rhs, preferred_element_type=F32
            )
            swept = value.astype(BF16).reshape(2, group, cells)
            out_ref[0, :, rows_of(b), block(q)] = swept
            fields.append(swept)
        return fields

    def receive(b):
        if b > 0:
            return receive_whole(b)
        def gathered(q, chosen):
            return turned_dot(q, chosen, [pieces[shifted(q, s)] for s in chosen])

        wait_edges(b)
        pieces = {q: piece(moved.at[b], q) for q in edges}
        left_over = {}
        for q in range(count):
            value = inner[:, rows_of(b), block(q)].reshape(2 * group, cells)
            chosen = [s for s in sides(q) if shifted(q, s) in pieces]
            left_over[q] = [s for s in sides(q) if s not in chosen]
            base[q] = value - gathered(q, chosen) if chosen else value
        wait_middle(b)
        pieces.update({q: piece(moved.at[b], q) for q in range(1, count - 1)})
        for q in range(count):
            if left_over[q]:
                base[q] -= gathered(q, left_over[q])
        wait_rims(b)
        part_waits(moved_part.at[b], move_part_sem, (b,), 1)
        coeff = coefficients(moved_part[b])
        fields = []
        for q in range(count):
            values, weights = [coeff], [left[:, block(q)]]
            for at, s, side in ((0, 1, 0), (count - 1, 2, 1)):
                if at == q:
                    values.append(stacked(moved_rim[b, side, 0], moved_rim[b, side, 1]))
                    weights.append(near_turned[q, pl.ds(s * 2 * cells, 2 * cells), :])
            value = base[q]
            for one, weight in zip(values, weights):
                value = value - jnp.dot(one, weight, preferred_element_type=F32)
            swept = value.astype(BF16).reshape(2, group, cells)
            out_ref[0, :, rows_of(b), block(q)] = swept
            fields.append(swept)
        return fields

    def emit(b, fields, first):
        coupled = []
        for q in range(count):
            value = (coupling_ref[:, block(q)].astype(F32)[None] * fields[q].astype(F32)).astype(BF16)
            sent[b, :, :, block(q)] = value
            coupled.append(value)
        def send_field():
            pl.when(has_high)(ahead_high(b).start)
            pl.when(has_low)(ahead_low(b).start)
            for copy in ahead_main(b):
                copy.start()

        early = first and b == 0
        if early:
            send_field()
        if b == 0:
            down.wait_recv()
        moved_part_sent[b] = folded([stacked(v[0], v[1]) for v in coupled], right_next)
        for copy in ahead_parts(b):
            copy.start()
        if not early:
            send_field()

    @pl.when(jnp.logical_not(has_prev))
    def _():
        for b in range(batches):
            out_ref[0, :, rows_of(b), :] = inner[:, rows_of(b), :].astype(BF16)

            @pl.when(has_next)
            def _():
                emit(b, [out_ref[0, :, rows_of(b), block(q)] for q in range(count)], True)

    @pl.when(has_prev & has_next)
    def _():
        for b in range(batches):
            emit(b, receive(b), False)

    @pl.when(has_prev & jnp.logical_not(has_next))
    def _():
        for b in range(batches):
            receive(b)

    pl.when(has_high)(to_high.wait_send)
    pl.when(has_low)(to_low.wait_send)
    part_waits(part, part_sem, (), 0)
    pl.when(has_prev)(down.wait_send)

    def drained(ref, index):
        pltpu.make_async_copy(ref, ref, sent_sem.at[index]).wait()

    @pl.when(has_next)
    def _():
        drained(sent, 0)
        pl.when(has_high)(lambda: drained(moved_rim.at[:, 0], 1))
        pl.when(has_low)(lambda: drained(moved_rim.at[:, 1], 2))
        for b in range(batches):
            part_waits(moved_part.at[b], move_part_sem, (b,), 0)


def body(layers, leafs, right_side, near_blocks, right_bases, left_bases, coupling, ranks):
    rows, width = right_side.shape[2:]
    cells = near_blocks.shape[-1]
    rank = right_bases.shape[3]
    count = width // cells
    batches = BATCHES
    group = rows // batches
    sources = leafs // 2 + leafs // 4
    dma = pltpu.SemaphoreType.DMA

    def fold_shape(size):
        height = max(4 * size * rank // TILE, 1)
        return (height, 4 * size * rank // height)

    return pl.pallas_call(
        functools.partial(kernel, layers, leafs, batches),
        out_shape=pltpu.VMEM(right_side.shape, BF16),
        in_specs=[pl.BlockSpec(memory_space=pl.ANY)] * 6,
        out_specs=pl.BlockSpec(memory_space=pltpu.VMEM),
        scratch_shapes=[
            pltpu.VMEM((2, rows, width), BF16),
            pltpu.VMEM((count, 3, 2, cells, cells), BF16),
            pltpu.VMEM((count, 6 * cells, cells), BF16),
            pltpu.VMEM((2, 2, rank, width), BF16),
            pltpu.VMEM((2, 2, rank, width), BF16),
            pltpu.VMEM((2, 2, rank, width), BF16),
            pltpu.VMEM((4 * rank, width), BF16),
            pltpu.VMEM(coupling.shape, BF16),
            pltpu.SMEM(ranks.shape, jnp.int32),
            pltpu.VMEM((2, rows, width), F32),
            pltpu.VMEM((count, 2 * group, cells), F32),
            pltpu.VMEM((2, 2, rows, cells), BF16),
            pltpu.VMEM((sources,) + fold_shape(rows), BF16),
            pltpu.VMEM(fold_shape(rows), BF16),
            pltpu.VMEM((batches, 2, group, width), BF16),
            pltpu.VMEM((batches, 2, group, width), BF16),
            pltpu.VMEM((batches, 2, 2, group, cells), BF16),
            pltpu.VMEM((batches, sources) + fold_shape(group), BF16),
            pltpu.VMEM((batches,) + fold_shape(group), BF16),
            dma((5,)),
            dma((count,)),
            dma((2, 2)),
            dma((2,)),
            dma((2,)),
            dma((batches, 2)),
            dma((batches, 2)),
            dma((2, batches)),
            dma((3,)),
            pltpu.SemaphoreType.REGULAR,
        ],
        compiler_params=pltpu.CompilerParams(collective_id=0, has_side_effects=True),
    )(right_side, near_blocks, right_bases, left_bases, coupling, ranks)


def solution(mesh):
    placed = (
        P("layer", None, None, "leaf"),
        P("layer", None, None, "leaf", None),
        P("layer", None, None, None, "leaf"),
        P("layer", None, None, None, "leaf"),
        P("layer", "leaf"),
        P("layer", None),
    )
    return jax.shard_map(
        functools.partial(body, mesh.shape["layer"], mesh.shape["leaf"]),
        mesh=mesh, in_specs=placed, out_specs=P("layer", None, None, "leaf"), check_vma=False,
    )
```

```python
import functools

import jax
import jax.numpy as jnp
from jax import lax
from jax.experimental import pallas as pl
from jax.experimental.pallas import tpu as pltpu
from jax.sharding import PartitionSpec as P

BATCHES = 4
TILE = 128
F32 = jnp.float32
BF16 = jnp.bfloat16
LANES = (((1,), (1,)), ((), ()))


def kernel(
    layers, leafs, batches,
    source_hbm, near_hbm, right_hbm, left_hbm, coupling_hbm, ranks_hbm,
    out_ref,
    source, near, near_turned, right, right_next, left_raw, left, coupling_ref, ranks_ref,
    inner, base, rim, part, part_sent, moved, sent, moved_rim, moved_part, moved_part_sent, early_sent,
    load_sem, rim_sem, part_sem, right_sem, move_sem, move_rim_sem, move_part_sem, sent_sem, ready_sem,
):
    layer = lax.axis_index("layer")
    leaf = lax.axis_index("leaf")
    rows, width = source.shape[1], source.shape[2]
    cells = near.shape[-1]
    count = width // cells
    rank = right.shape[2]
    group = rows // batches
    half, quarter = leafs // 2, leafs // 4
    upper, lower = leaf // half, leaf // quarter
    has_low, has_high = leaf > 0, leaf < leafs - 1
    has_prev, has_next = layer > 0, layer < layers - 1
    edges = [0, count - 1] if count > 1 else [0]

    def remote(src, dst, sems, index, to_layer, to_leaf):
        return pltpu.make_async_remote_copy(
            src_ref=src, dst_ref=dst,
            send_sem=sems.at[(0,) + index],
            recv_sem=sems.at[(1,) + index],
            device_id=(to_layer, to_leaf), device_id_type=pl.DeviceIdType.MESH,
        )

    barrier = pltpu.get_barrier_semaphore()

    def greet(to_layer, to_leaf):
        pl.semaphore_signal(
            barrier, inc=1, device_id=(to_layer, to_leaf), device_id_type=pl.DeviceIdType.MESH
        )

    for step in range(1, leafs):
        greet(layer, lax.rem(leaf + step, leafs))

    pl.when(has_prev)(lambda: greet(layer - 1, leaf))
    pl.when(has_next)(lambda: greet(layer + 1, leaf))

    loads = [
        pltpu.make_async_copy(source_hbm.at[0], source, load_sem.at[0]),
        pltpu.make_async_copy(right_hbm.at[0], right, load_sem.at[1]),
        pltpu.make_async_copy(left_hbm.at[0], left_raw, load_sem.at[2]),
        pltpu.make_async_copy(coupling_hbm, coupling_ref, load_sem.at[3]),
        pltpu.make_async_copy(ranks_hbm, ranks_ref, load_sem.at[4]),
    ]
    near_loads = [
        pltpu.make_async_copy(
            near_hbm.at[0, :, :, pl.ds(q * cells, cells), :], near.at[q], load_sem.at[5]
        )
        for q in range(count)
    ]
    for copy in loads + near_loads:
        copy.start()

    @pl.when(jnp.logical_not(has_low))
    def _():
        rim[0] = jnp.zeros(rim.shape[1:], BF16)
        for b in range(batches):
            moved_rim[b, 0] = jnp.zeros(moved_rim.shape[2:], BF16)

    @pl.when(jnp.logical_not(has_high))
    def _():
        rim[1] = jnp.zeros(rim.shape[1:], BF16)
        for b in range(batches):
            moved_rim[b, 1] = jnp.zeros(moved_rim.shape[2:], BF16)

    def block(q):
        return pl.ds(q * cells, cells)

    def stacked(real, imag):
        return jnp.concatenate(
            [
                jnp.concatenate([real, imag], axis=0),
                jnp.concatenate([-imag, real], axis=0),
            ],
            axis=1,
        )

    def piece(field, q):
        return stacked(field[0, :, block(q)], field[1, :, block(q)])

    def sides(q):
        return [0] + ([1] if q > 0 else []) + ([2] if q < count - 1 else [])

    def shifted(q, s):
        return q + (0, -1, 1)[s]

    def level_sums(pieces, bases):
        flat = [bases[c, :, block(q)] for q in range(count) for c in range(2)]
        return lax.dot_general(
            jnp.concatenate(pieces, axis=1), jnp.concatenate(flat, axis=1), LANES,
            preferred_element_type=F32,
        )

    def folded(pieces, bases):
        flat = [
            bases[:, c, :, block(q)].reshape(2 * rank, cells) for q in range(count) for c in range(2)
        ]
        total = lax.dot_general(
            jnp.concatenate(pieces, axis=1), jnp.concatenate(flat, axis=1), LANES,
            preferred_element_type=F32,
        )
        return packed(total)

    def packed(total):
        height = max(total.shape[0] * total.shape[1] // TILE, 1)
        return jnp.concatenate(
            [total[at:at + height] for at in range(0, total.shape[0], height)], axis=1
        ).astype(BF16)

    def part_copies(src, dst, sems, index, to_layer):
        copies = []
        slot = lax.rem(leaf, half)
        for other in range(half):
            copies.append(remote(
                src, dst.at[slot], sems, index,
                to_layer, (1 - upper) * half + other,
            ))
        slot = half + lax.rem(leaf, quarter)
        sibling = lower + 1 - 2 * lax.rem(lower, 2)
        for other in range(quarter):
            copies.append(remote(
                src, dst.at[slot], sems, index,
                to_layer, sibling * quarter + other,
            ))
        return copies

    def part_waits(dst, sems, index, way):
        pltpu.make_async_copy(dst, dst, sems.at[(way,) + index]).wait()

    def coefficients(parts):
        first = parts[0].astype(F32)
        for slot in range(1, half):
            first = first + parts[slot].astype(F32)
        second = parts[half].astype(F32)
        for slot in range(1, quarter):
            second = second + parts[half + slot].astype(F32)
        column = lax.broadcasted_iota(jnp.int32, first.shape, 1)
        both = jnp.where(lax.rem(column, 2 * rank) < rank, first, second)
        turned = jnp.concatenate(
            [both[:, at:at + 2 * rank] for at in range(0, both.shape[1], 2 * rank)], axis=0
        )
        size = turned.shape[0] // 2
        swapped = jnp.concatenate([-turned[size:], turned[:size]], axis=0)
        return jnp.concatenate([turned, swapped], axis=1).astype(BF16)

    def far_leaf(q, coeff):
        return jnp.dot(coeff, left[:, block(q)], preferred_element_type=F32)

    def plain_dot(q, s, value):
        rhs = jnp.concatenate([near[q, s, 0], near[q, s, 1]], axis=1)
        return lax.dot_general(value, rhs, LANES, preferred_element_type=F32)

    def turned_dot(q, chosen, values):
        rhs = [near_turned[q, pl.ds(s * 2 * cells, 2 * cells), :] for s in chosen]
        return jnp.dot(
            jnp.concatenate(values, axis=1), jnp.concatenate(rhs, axis=0),
            preferred_element_type=F32,
        )

    loads[0].wait()
    loads[1].wait()
    source_pieces = [piece(source, q) for q in range(count)]
    part_sent[...] = folded(source_pieces, right)

    pl.semaphore_wait(
        barrier, leafs - 1 + has_prev.astype(jnp.int32) + has_next.astype(jnp.int32)
    )

    downs = [
        remote(right.at[level], right_next.at[level], right_sem, (level,), layer - 1, leaf)
        for level in range(2)
    ]

    @pl.when(has_prev)
    def _():
        for copy in downs:
            copy.start()

    to_high = remote(
        source.at[:, :, block(count - 1)], rim.at[0], rim_sem, (0,), layer, leaf + 1
    )
    to_low = remote(source.at[:, :, block(0)], rim.at[1], rim_sem, (1,), layer, leaf - 1)
    source_parts = part_copies(part_sent, part, part_sem, (), layer)

    @pl.when(has_prev)
    def _():
        pl.semaphore_signal(
            ready_sem, inc=1, device_id=(layer - 1, leaf), device_id_type=pl.DeviceIdType.MESH
        )

    for copy in source_parts:
        copy.start()
    pl.when(has_high)(to_high.start)
    pl.when(has_low)(to_low.start)

    loads[2].wait()
    loads[3].wait()
    loads[4].wait()
    row_ids = lax.broadcasted_iota(jnp.int32, (rank, width), 0)
    for level, slot in ((0, upper), (1, 2 + lower)):
        keep = (row_ids < ranks_ref[0, slot]).astype(F32)
        for c in range(2):
            left[pl.ds((2 * c + level) * rank, rank), :] = (
                left_raw[level, c].astype(F32) * keep
            ).astype(BF16)

    pltpu.make_async_copy(near, near, load_sem.at[5]).wait()
    for q in range(count):
        value = None
        for s in sides(q):
            term = plain_dot(q, s, source_pieces[shifted(q, s)])
            value = term if value is None else value + term
        inner[:, :, block(q)] = value.reshape(2, rows, cells)
    pl.when(has_low)(to_high.wait_recv)
    pl.when(has_high)(to_low.wait_recv)
    for q, s, side in ((0, 1, 0), (count - 1, 2, 1)):
        inner[:, :, block(q)] += plain_dot(q, s, stacked(rim[side, 0], rim[side, 1])).reshape(
            2, rows, cells
        )
    part_waits(part, part_sem, (), 1)
    coeff = coefficients(part)
    for q in range(count):
        inner[:, :, block(q)] += far_leaf(q, coeff).reshape(2, rows, cells)

    @pl.when(has_prev)
    def _():
        for q in range(count):
            for s in range(3):
                for c in range(2):
                    near_turned[q, pl.ds((2 * s + c) * cells, cells), :] = near[q, s, c].T

    pl.when(has_next)(lambda: pl.semaphore_wait(ready_sem, 1))

    def rows_of(b):
        return pl.ds(b * group, group)

    def ahead_main(b):
        pairs = [(block(q), 0) for q in edges]
        if count > 2:
            pairs.append((pl.ds(cells, width - 2 * cells), 1))
        return [
            pltpu.make_async_remote_copy(
                src_ref=sent.at[b, :, :, span], dst_ref=moved.at[b, :, :, span],
                send_sem=sent_sem.at[0], recv_sem=move_sem.at[b, kind],
                device_id=(layer + 1, leaf), device_id_type=pl.DeviceIdType.MESH,
            )
            for span, kind in pairs
        ]

    def rim_copy(source_ref, q, b, side, to_layer, to_leaf):
        return pltpu.make_async_remote_copy(
            src_ref=source_ref.at[b, :, :, block(q)], dst_ref=moved_rim.at[b, side],
            send_sem=sent_sem.at[1 + side], recv_sem=move_rim_sem.at[b, side],
            device_id=(to_layer, to_leaf), device_id_type=pl.DeviceIdType.MESH,
        )

    def ahead_high(b):
        return rim_copy(sent, count - 1, b, 0, layer + 1, leaf + 1)

    def ahead_low(b):
        return rim_copy(sent, 0, b, 1, layer + 1, leaf - 1)

    def ahead_parts(b):
        return part_copies(
            moved_part_sent.at[b], moved_part.at[b], move_part_sem, (b,), layer + 1
        )

    def early_parts():
        return part_copies(
            early_sent, moved_part.at[0], move_part_sem, (0,), layer + 1
        )[:half]

    def wait_edges(b):
        view = moved.at[b, :, :, pl.ds(0, len(edges) * cells)]
        pltpu.make_async_copy(view, view, move_sem.at[b, 0]).wait()

    def wait_middle(b):
        if count > 2:
            view = moved.at[b, :, :, pl.ds(cells, width - 2 * cells)]
            pltpu.make_async_copy(view, view, move_sem.at[b, 1]).wait()

    def wait_rims(b):
        pl.when(has_low)(ahead_high(b).wait_recv)
        pl.when(has_high)(ahead_low(b).wait_recv)

    def receive_whole(b):
        wait_edges(b)
        wait_middle(b)
        wait_rims(b)
        part_waits(moved_part.at[b], move_part_sem, (b,), 1)
        coeff = coefficients(moved_part[b])
        pieces = [stacked(moved_rim[b, 0, 0], moved_rim[b, 0, 1])]
        pieces += [piece(moved.at[b], q) for q in range(count)]
        pieces += [stacked(moved_rim[b, 1, 0], moved_rim[b, 1, 1])]
        fields = []
        for q in range(count):
            lhs = jnp.concatenate([pieces[q + 1], pieces[q], pieces[q + 2], coeff], axis=1)
            rhs = jnp.concatenate([near_turned[q], left[:, block(q)]], axis=0)
            value = inner[:, rows_of(b), block(q)].reshape(2 * group, cells) - jnp.dot(
                lhs, rhs, preferred_element_type=F32
            )
            swept = value.astype(BF16).reshape(2, group, cells)
            out_ref[0, :, rows_of(b), block(q)] = swept
            fields.append(swept)
        return fields

    def receive(b, staged):
        if not staged:
            return receive_whole(b)
        def gathered(q, chosen):
            return turned_dot(q, chosen, [pieces[shifted(q, s)] for s in chosen])

        wait_edges(b)
        pieces = {q: piece(moved.at[b], q) for q in edges}
        left_over = {}
        for q in range(count):
            value = inner[:, rows_of(b), block(q)].reshape(2 * group, cells)
            chosen = [s for s in sides(q) if shifted(q, s) in pieces]
            left_over[q] = [s for s in sides(q) if s not in chosen]
            base[q] = value - gathered(q, chosen) if chosen else value
        wait_middle(b)
        pieces.update({q: piece(moved.at[b], q) for q in range(1, count - 1)})
        for q in range(count):
            if left_over[q]:
                base[q] -= gathered(q, left_over[q])
        wait_rims(b)
        part_waits(moved_part.at[b], move_part_sem, (b,), 1)
        coeff = coefficients(moved_part[b])
        fields = []
        for q in range(count):
            values, weights = [coeff], [left[:, block(q)]]
            for at, s, side in ((0, 1, 0), (count - 1, 2, 1)):
                if at == q:
                    values.append(stacked(moved_rim[b, side, 0], moved_rim[b, side, 1]))
                    weights.append(near_turned[q, pl.ds(s * 2 * cells, 2 * cells), :])
            value = base[q]
            for one, weight in zip(values, weights):
                value = value - jnp.dot(one, weight, preferred_element_type=F32)
            swept = value.astype(BF16).reshape(2, group, cells)
            out_ref[0, :, rows_of(b), block(q)] = swept
            fields.append(swept)
        return fields

    def couple(b, fields):
        coupled = []
        for q in range(count):
            value = (coupling_ref[:, block(q)].astype(F32)[None] * fields[q].astype(F32)).astype(BF16)
            sent[b, :, :, block(q)] = value
            coupled.append(stacked(value[0], value[1]))
        return coupled

    def send_rims(b):
        pl.when(has_high)(ahead_high(b).start)
        pl.when(has_low)(ahead_low(b).start)

    def send_main(b):
        for copy in ahead_main(b):
            copy.start()

    def send_field(b):
        send_rims(b)
        send_main(b)

    def send_parts(b, stacks):
        moved_part_sent[b] = folded(stacks, right_next)
        for copy in ahead_parts(b):
            copy.start()

    def emit_first():
        for b in range(batches):
            couple(b, [out_ref[0, :, rows_of(b), block(q)] for q in range(count)])
            if b == 0:
                send_field(b)
        stacks = [piece(sent.at[0], q) for q in range(count)]
        downs[0].wait_recv()
        first_level = level_sums(stacks, right_next.at[0])
        early_sent[...] = packed(
            jnp.concatenate([first_level, jnp.zeros_like(first_level)], axis=1)
        )
        for copy in early_parts():
            copy.start()
        if batches > 1:
            send_main(1)
        downs[1].wait_recv()
        second_level = level_sums(stacks, right_next.at[1])
        moved_part_sent[0] = packed(jnp.concatenate([first_level, second_level], axis=1))
        for copy in ahead_parts(0)[half:]:
            copy.start()
        if batches > 1:
            send_rims(1)
        for b in range(1, batches):
            send_parts(b, [piece(sent.at[b], q) for q in range(count)])
            if b > 1:
                send_field(b)

    @pl.when(jnp.logical_not(has_prev))
    def _():
        out_ref[0] = inner[...].astype(BF16)
        pl.when(has_next)(emit_first)

    @pl.when(has_prev & has_next)
    def _():
        for b in range(batches):
            if b == 0:
                for copy in downs:
                    copy.wait_recv()
            stacks = couple(b, receive(b, b == 0))
            send_parts(b, stacks)
            send_field(b)

    @pl.when(has_prev & jnp.logical_not(has_next))
    def _():
        for b in range(batches):
            receive(b, b == 0)

    pl.when(has_high)(to_high.wait_send)
    pl.when(has_low)(to_low.wait_send)
    part_waits(part, part_sem, (), 0)

    @pl.when(has_prev)
    def _():
        for copy in downs:
            copy.wait_send()


    def drained(ref, index):
        pltpu.make_async_copy(ref, ref, sent_sem.at[index]).wait()

    @pl.when(has_next)
    def _():
        drained(sent, 0)
        pl.when(has_high)(lambda: drained(moved_rim.at[:, 0], 1))
        pl.when(has_low)(lambda: drained(moved_rim.at[:, 1], 2))
        for b in range(batches):
            part_waits(moved_part.at[b], move_part_sem, (b,), 0)


def body(layers, leafs, right_side, near_blocks, right_bases, left_bases, coupling, ranks):
    rows, width = right_side.shape[2:]
    cells = near_blocks.shape[-1]
    rank = right_bases.shape[3]
    count = width // cells
    batches = BATCHES
    group = rows // batches
    sources = leafs // 2 + leafs // 4
    dma = pltpu.SemaphoreType.DMA

    def fold_shape(size):
        height = max(4 * size * rank // TILE, 1)
        return (height, 4 * size * rank // height)

    return pl.pallas_call(
        functools.partial(kernel, layers, leafs, batches),
        out_shape=pltpu.VMEM(right_side.shape, BF16),
        in_specs=[pl.BlockSpec(memory_space=pl.ANY)] * 6,
        out_specs=pl.BlockSpec(memory_space=pltpu.VMEM),
        scratch_shapes=[
            pltpu.VMEM((2, rows, width), BF16),
            pltpu.VMEM((count, 3, 2, cells, cells), BF16),
            pltpu.VMEM((count, 6 * cells, cells), BF16),
            pltpu.VMEM((2, 2, rank, width), BF16),
            pltpu.VMEM((2, 2, rank, width), BF16),
            pltpu.VMEM((2, 2, rank, width), BF16),
            pltpu.VMEM((4 * rank, width), BF16),
            pltpu.VMEM(coupling.shape, BF16),
            pltpu.SMEM(ranks.shape, jnp.int32),
            pltpu.VMEM((2, rows, width), F32),
            pltpu.VMEM((count, 2 * group, cells), F32),
            pltpu.VMEM((2, 2, rows, cells), BF16),
            pltpu.VMEM((sources,) + fold_shape(rows), BF16),
            pltpu.VMEM(fold_shape(rows), BF16),
            pltpu.VMEM((batches, 2, group, width), BF16),
            pltpu.VMEM((batches, 2, group, width), BF16),
            pltpu.VMEM((batches, 2, 2, group, cells), BF16),
            pltpu.VMEM((batches, sources) + fold_shape(group), BF16),
            pltpu.VMEM((batches,) + fold_shape(group), BF16),
            pltpu.VMEM(fold_shape(group), BF16),
            dma((6,)),
            dma((2, 2)),
            dma((2,)),
            dma((2, 2)),
            dma((batches, 2)),
            dma((batches, 2)),
            dma((2, batches)),
            dma((3,)),
            pltpu.SemaphoreType.REGULAR,
        ],
        compiler_params=pltpu.CompilerParams(collective_id=0, has_side_effects=True),
    )(right_side, near_blocks, right_bases, left_bases, coupling, ranks)


def solution(mesh):
    placed = (
        P("layer", None, None, "leaf"),
        P("layer", None, None, "leaf", None),
        P("layer", None, None, None, "leaf"),
        P("layer", None, None, None, "leaf"),
        P("layer", "leaf"),
        P("layer", None),
    )
    return jax.shard_map(
        functools.partial(body, mesh.shape["layer"], mesh.shape["leaf"]),
        mesh=mesh, in_specs=placed, out_specs=P("layer", None, None, "leaf"), check_vma=False,
    )
```

```python
import functools

import jax
import jax.numpy as jnp
from jax import lax
from jax.experimental import pallas as pl
from jax.experimental.pallas import tpu as pltpu
from jax.sharding import PartitionSpec as P

BATCHES = 4
TILE = 128
F32 = jnp.float32
BF16 = jnp.bfloat16
LANES = (((1,), (1,)), ((), ()))


def kernel(
    layers, leafs, batches,
    source_hbm, near_hbm, right_hbm, left_hbm, coupling_hbm, ranks_hbm,
    out_ref,
    source, near, near_turned, right, right_next, left_raw, left, coupling_ref, ranks_ref,
    inner, base, rim, part, part_sent, moved, sent, moved_rim, moved_part, moved_part_sent,
    load_sem, rim_sem, part_sem, right_sem, move_sem, move_rim_sem, move_part_sem, sent_sem, ready_sem,
):
    layer = lax.axis_index("layer")
    leaf = lax.axis_index("leaf")
    rows, width = source.shape[1], source.shape[2]
    cells = near.shape[-1]
    count = width // cells
    rank = right.shape[2]
    group = rows // batches
    half, quarter = leafs // 2, leafs // 4
    upper, lower = leaf // half, leaf // quarter
    has_low, has_high = leaf > 0, leaf < leafs - 1
    odd, even = lax.rem(leaf, 2) == 1, lax.rem(leaf, 2) == 0
    has_prev, has_next = layer > 0, layer < layers - 1
    edges = [0, count - 1] if count > 1 else [0]

    def remote(src, dst, sems, index, to_layer, to_leaf):
        return pltpu.make_async_remote_copy(
            src_ref=src, dst_ref=dst,
            send_sem=sems.at[(0,) + index],
            recv_sem=sems.at[(1,) + index],
            device_id=(to_layer, to_leaf), device_id_type=pl.DeviceIdType.MESH,
        )

    barrier = pltpu.get_barrier_semaphore()

    def greet(to_layer, to_leaf):
        pl.semaphore_signal(
            barrier, inc=1, device_id=(to_layer, to_leaf), device_id_type=pl.DeviceIdType.MESH
        )

    for step in range(1, leafs):
        greet(layer, lax.rem(leaf + step, leafs))

    pl.when(has_prev)(lambda: greet(layer - 1, leaf))
    pl.when(has_next)(lambda: greet(layer + 1, leaf))

    loads = [
        pltpu.make_async_copy(source_hbm.at[0], source, load_sem.at[0]),
        pltpu.make_async_copy(right_hbm.at[0], right, load_sem.at[1]),
        pltpu.make_async_copy(left_hbm.at[0], left_raw, load_sem.at[2]),
        pltpu.make_async_copy(coupling_hbm, coupling_ref, load_sem.at[3]),
        pltpu.make_async_copy(ranks_hbm, ranks_ref, load_sem.at[4]),
    ]
    near_loads = [
        pltpu.make_async_copy(
            near_hbm.at[0, :, :, pl.ds(q * cells, cells), :], near.at[q], load_sem.at[5]
        )
        for q in range(count)
    ]
    for copy in loads + near_loads:
        copy.start()

    @pl.when(jnp.logical_not(has_low))
    def _():
        rim[0] = jnp.zeros(rim.shape[1:], BF16)
        for b in range(batches):
            moved_rim[b, 0] = jnp.zeros(moved_rim.shape[2:], BF16)

    @pl.when(jnp.logical_not(has_high))
    def _():
        rim[1] = jnp.zeros(rim.shape[1:], BF16)
        for b in range(batches):
            moved_rim[b, 1] = jnp.zeros(moved_rim.shape[2:], BF16)

    def block(q):
        return pl.ds(q * cells, cells)

    def stacked(real, imag):
        return jnp.concatenate(
            [
                jnp.concatenate([real, imag], axis=0),
                jnp.concatenate([-imag, real], axis=0),
            ],
            axis=1,
        )

    def piece(field, q):
        return stacked(field[0, :, block(q)], field[1, :, block(q)])

    def sides(q):
        return [0] + ([1] if q > 0 else []) + ([2] if q < count - 1 else [])

    def shifted(q, s):
        return q + (0, -1, 1)[s]

    def level_sums(pieces, bases):
        flat = [bases[c, :, block(q)] for q in range(count) for c in range(2)]
        return lax.dot_general(
            jnp.concatenate(pieces, axis=1), jnp.concatenate(flat, axis=1), LANES,
            preferred_element_type=F32,
        )

    def folded(pieces, bases):
        flat = [
            bases[:, c, :, block(q)].reshape(2 * rank, cells) for q in range(count) for c in range(2)
        ]
        total = lax.dot_general(
            jnp.concatenate(pieces, axis=1), jnp.concatenate(flat, axis=1), LANES,
            preferred_element_type=F32,
        )
        return [packed(total[:, level * rank:(level + 1) * rank]) for level in range(2)]

    def packed(total):
        height = max(total.shape[0] * total.shape[1] // TILE, 1)
        return jnp.concatenate(
            [total[at:at + height] for at in range(0, total.shape[0], height)], axis=1
        ).astype(BF16)

    def part_copies(src, dst, sems, index, to_layer):
        copies = []
        slot = lax.rem(leaf, half)
        for other in range(half):
            copies.append(remote(
                src.at[0], dst.at[slot], sems, index,
                to_layer, (1 - upper) * half + other,
            ))
        slot = half + lax.rem(leaf, quarter)
        sibling = lower + 1 - 2 * lax.rem(lower, 2)
        for other in range(quarter):
            copies.append(remote(
                src.at[1], dst.at[slot], sems, index,
                to_layer, sibling * quarter + other,
            ))
        return copies

    def part_waits(dst, sems, index, way):
        pltpu.make_async_copy(dst, dst, sems.at[(way,) + index]).wait()

    def coefficients(parts):
        first = parts[0].astype(F32)
        for slot in range(1, half):
            first = first + parts[slot].astype(F32)
        second = parts[half].astype(F32)
        for slot in range(1, quarter):
            second = second + parts[half + slot].astype(F32)
        def unpacked(flat):
            return jnp.concatenate(
                [flat[:, at:at + rank] for at in range(0, flat.shape[1], rank)], axis=0
            )

        turned = jnp.concatenate([unpacked(first), unpacked(second)], axis=1)
        size = turned.shape[0] // 2
        swapped = jnp.concatenate([-turned[size:], turned[:size]], axis=0)
        return jnp.concatenate([turned, swapped], axis=1).astype(BF16)

    def far_leaf(q, coeff):
        return jnp.dot(coeff, left[:, block(q)], preferred_element_type=F32)

    def plain_dot(q, s, value):
        rhs = jnp.concatenate([near[q, s, 0], near[q, s, 1]], axis=1)
        return lax.dot_general(value, rhs, LANES, preferred_element_type=F32)

    def turned_dot(q, chosen, values):
        rhs = [near_turned[q, pl.ds(s * 2 * cells, 2 * cells), :] for s in chosen]
        return jnp.dot(
            jnp.concatenate(values, axis=1), jnp.concatenate(rhs, axis=0),
            preferred_element_type=F32,
        )

    loads[0].wait()
    loads[1].wait()
    source_pieces = [piece(source, q) for q in range(count)]
    part_sent[0], part_sent[1] = folded(source_pieces, right)

    pl.semaphore_wait(
        barrier, leafs - 1 + has_prev.astype(jnp.int32) + has_next.astype(jnp.int32)
    )

    downs = [
        remote(right.at[level], right_next.at[level], right_sem, (level,), layer - 1, leaf)
        for level in range(2)
    ]

    @pl.when(has_prev)
    def _():
        for copy in downs:
            copy.start()

    to_high = remote(
        source.at[:, :, block(count - 1)], rim.at[0], rim_sem, (0,), layer, leaf + 1
    )
    to_low = remote(source.at[:, :, block(0)], rim.at[1], rim_sem, (1,), layer, leaf - 1)
    source_parts = part_copies(part_sent, part, part_sem, (), layer)

    @pl.when(has_prev)
    def _():
        pl.semaphore_signal(
            ready_sem, inc=1, device_id=(layer - 1, leaf), device_id_type=pl.DeviceIdType.MESH
        )

    for copy in source_parts:
        copy.start()
    pl.when(has_high)(to_high.start)
    pl.when(has_low)(to_low.start)

    loads[2].wait()
    loads[3].wait()
    loads[4].wait()
    row_ids = lax.broadcasted_iota(jnp.int32, (rank, width), 0)
    for level, slot in ((0, upper), (1, 2 + lower)):
        keep = (row_ids < ranks_ref[0, slot]).astype(F32)
        for c in range(2):
            left[pl.ds((2 * c + level) * rank, rank), :] = (
                left_raw[level, c].astype(F32) * keep
            ).astype(BF16)

    pltpu.make_async_copy(near, near, load_sem.at[5]).wait()
    for q in range(count):
        value = None
        for s in sides(q):
            term = plain_dot(q, s, source_pieces[shifted(q, s)])
            value = term if value is None else value + term
        inner[:, :, block(q)] = value.reshape(2, rows, cells)
    pl.when(has_low)(to_high.wait_recv)
    pl.when(has_high)(to_low.wait_recv)
    for q, s, side in ((0, 1, 0), (count - 1, 2, 1)):
        inner[:, :, block(q)] += plain_dot(q, s, stacked(rim[side, 0], rim[side, 1])).reshape(
            2, rows, cells
        )
    part_waits(part, part_sem, (), 1)
    coeff = coefficients(part)
    for q in range(count):
        inner[:, :, block(q)] += far_leaf(q, coeff).reshape(2, rows, cells)

    @pl.when(has_prev)
    def _():
        for q in range(count):
            for s in range(3):
                for c in range(2):
                    near_turned[q, pl.ds((2 * s + c) * cells, cells), :] = near[q, s, c].T

    pl.when(has_next)(lambda: pl.semaphore_wait(ready_sem, 1))

    def rows_of(b):
        return pl.ds(b * group, group)

    def ahead_main(b):
        pairs = [(block(q), 0) for q in edges]
        if count > 2:
            pairs.append((pl.ds(cells, width - 2 * cells), 1))
        return [
            pltpu.make_async_remote_copy(
                src_ref=sent.at[b, :, :, span], dst_ref=moved.at[b, :, :, span],
                send_sem=sent_sem.at[0], recv_sem=move_sem.at[b, kind],
                device_id=(layer + 1, leaf), device_id_type=pl.DeviceIdType.MESH,
            )
            for span, kind in pairs
        ]

    def rim_copy(source_ref, q, b, side, to_layer, to_leaf):
        return pltpu.make_async_remote_copy(
            src_ref=source_ref.at[b, :, :, block(q)], dst_ref=moved_rim.at[b, side],
            send_sem=sent_sem.at[1 + side], recv_sem=move_rim_sem.at[b, side],
            device_id=(to_layer, to_leaf), device_id_type=pl.DeviceIdType.MESH,
        )

    def ahead_high(b):
        return rim_copy(sent, count - 1, b, 0, layer + 1, leaf + 1)

    def ahead_low(b):
        return rim_copy(sent, 0, b, 1, layer + 1, leaf - 1)

    def across_low(b):
        return pltpu.make_async_remote_copy(
            src_ref=moved.at[b, :, :, block(0)], dst_ref=moved_rim.at[b, 1],
            send_sem=sent_sem.at[3], recv_sem=move_rim_sem.at[b, 1],
            device_id=(layer, leaf - 1), device_id_type=pl.DeviceIdType.MESH,
        )

    def hand_across(b):
        if b < batches:

            @pl.when(odd)
            def _():
                wait_edges(b)
                across_low(b).start()

    def ahead_parts(b):
        return part_copies(
            moved_part_sent.at[b], moved_part.at[b], move_part_sem, (b,), layer + 1
        )


    def wait_edges(b):
        view = moved.at[b, :, :, pl.ds(0, len(edges) * cells)]
        pltpu.make_async_copy(view, view, move_sem.at[b, 0]).wait()

    def wait_middle(b):
        if count > 2:
            view = moved.at[b, :, :, pl.ds(cells, width - 2 * cells)]
            pltpu.make_async_copy(view, view, move_sem.at[b, 1]).wait()

    def wait_rims(b):
        pl.when(has_low)(ahead_high(b).wait_recv)
        pl.when(has_high)(ahead_low(b).wait_recv)

    def receive_whole(b):
        pl.when(even)(lambda: wait_edges(b))
        wait_middle(b)
        wait_rims(b)
        part_waits(moved_part.at[b], move_part_sem, (b,), 1)
        hand_across(b + 1)
        coeff = coefficients(moved_part[b])
        pieces = [stacked(moved_rim[b, 0, 0], moved_rim[b, 0, 1])]
        pieces += [piece(moved.at[b], q) for q in range(count)]
        pieces += [stacked(moved_rim[b, 1, 0], moved_rim[b, 1, 1])]
        fields = []
        for q in range(count):
            lhs = jnp.concatenate([pieces[q + 1], pieces[q], pieces[q + 2], coeff], axis=1)
            rhs = jnp.concatenate([near_turned[q], left[:, block(q)]], axis=0)
            value = inner[:, rows_of(b), block(q)].reshape(2 * group, cells) - jnp.dot(
                lhs, rhs, preferred_element_type=F32
            )
            swept = value.astype(BF16).reshape(2, group, cells)
            out_ref[0, :, rows_of(b), block(q)] = swept
            fields.append(swept)
        return fields

    def receive(b, staged):
        if not staged:
            return receive_whole(b)
        def gathered(q, chosen):
            return turned_dot(q, chosen, [pieces[shifted(q, s)] for s in chosen])

        hand_across(b)
        pl.when(even)(lambda: wait_edges(b))
        pieces = {q: piece(moved.at[b], q) for q in edges}
        left_over = {}
        for q in range(count):
            value = inner[:, rows_of(b), block(q)].reshape(2 * group, cells)
            chosen = [s for s in sides(q) if shifted(q, s) in pieces]
            left_over[q] = [s for s in sides(q) if s not in chosen]
            base[q] = value - gathered(q, chosen) if chosen else value
        wait_middle(b)
        pieces.update({q: piece(moved.at[b], q) for q in range(1, count - 1)})
        for q in range(count):
            if left_over[q]:
                base[q] -= gathered(q, left_over[q])
        wait_rims(b)
        hand_across(b + 1)
        part_waits(moved_part.at[b], move_part_sem, (b,), 1)
        coeff = coefficients(moved_part[b])
        fields = []
        for q in range(count):
            values, weights = [coeff], [left[:, block(q)]]
            for at, s, side in ((0, 1, 0), (count - 1, 2, 1)):
                if at == q:
                    values.append(stacked(moved_rim[b, side, 0], moved_rim[b, side, 1]))
                    weights.append(near_turned[q, pl.ds(s * 2 * cells, 2 * cells), :])
            value = base[q]
            for one, weight in zip(values, weights):
                value = value - jnp.dot(one, weight, preferred_element_type=F32)
            swept = value.astype(BF16).reshape(2, group, cells)
            out_ref[0, :, rows_of(b), block(q)] = swept
            fields.append(swept)
        return fields

    def couple(b, fields):
        coupled = []
        for q in range(count):
            value = (coupling_ref[:, block(q)].astype(F32)[None] * fields[q].astype(F32)).astype(BF16)
            sent[b, :, :, block(q)] = value
            coupled.append(stacked(value[0], value[1]))
        return coupled

    def send_rims(b):
        pl.when(has_high)(ahead_high(b).start)
        pl.when(even & has_low)(ahead_low(b).start)

    def send_main(b):
        for copy in ahead_main(b):
            copy.start()

    def send_field(b):
        send_rims(b)
        send_main(b)

    def send_parts(b, stacks):
        moved_part_sent[b, 0], moved_part_sent[b, 1] = folded(stacks, right_next)
        for copy in ahead_parts(b):
            copy.start()

    def emit_first():
        for b in range(batches):
            couple(b, [out_ref[0, :, rows_of(b), block(q)] for q in range(count)])
            if b == 0:
                send_field(b)
        stacks = [piece(sent.at[0], q) for q in range(count)]
        downs[0].wait_recv()
        moved_part_sent[0, 0] = packed(level_sums(stacks, right_next.at[0]))
        for copy in ahead_parts(0)[:half]:
            copy.start()
        if batches > 1:
            send_main(1)
        downs[1].wait_recv()
        moved_part_sent[0, 1] = packed(level_sums(stacks, right_next.at[1]))
        for copy in ahead_parts(0)[half:]:
            copy.start()
        if batches > 1:
            send_rims(1)
        for b in range(1, batches):
            send_parts(b, [piece(sent.at[b], q) for q in range(count)])
            if b > 1:
                send_field(b)

    @pl.when(jnp.logical_not(has_prev))
    def _():
        out_ref[0] = inner[...].astype(BF16)
        pl.when(has_next)(emit_first)

    @pl.when(has_prev & has_next)
    def _():
        for b in range(batches):
            if b == 0:
                for copy in downs:
                    copy.wait_recv()
            stacks = couple(b, receive(b, b == 0))
            send_rims(b)
            send_parts(b, stacks)
            send_main(b)

    @pl.when(has_prev & jnp.logical_not(has_next))
    def _():
        for b in range(batches):
            receive(b, b == 0)

    pl.when(has_high)(to_high.wait_send)
    pl.when(has_low)(to_low.wait_send)
    part_waits(part, part_sem, (), 0)

    @pl.when(has_prev)
    def _():
        for copy in downs:
            copy.wait_send()


    def drained(ref, index):
        pltpu.make_async_copy(ref, ref, sent_sem.at[index]).wait()

    pl.when(has_prev & odd)(lambda: drained(moved_rim.at[:, 1], 3))

    @pl.when(has_next)
    def _():
        drained(sent, 0)
        pl.when(has_high)(lambda: drained(moved_rim.at[:, 0], 1))
        pl.when(even & has_low)(lambda: drained(moved_rim.at[:, 1], 2))
        for b in range(batches):
            part_waits(moved_part.at[b], move_part_sem, (b,), 0)


def body(layers, leafs, right_side, near_blocks, right_bases, left_bases, coupling, ranks):
    rows, width = right_side.shape[2:]
    cells = near_blocks.shape[-1]
    rank = right_bases.shape[3]
    count = width // cells
    batches = BATCHES
    group = rows // batches
    sources = leafs // 2 + leafs // 4
    dma = pltpu.SemaphoreType.DMA

    def fold_shape(size):
        height = max(2 * size * rank // TILE, 1)
        return (height, 2 * size * rank // height)

    return pl.pallas_call(
        functools.partial(kernel, layers, leafs, batches),
        out_shape=pltpu.VMEM(right_side.shape, BF16),
        in_specs=[pl.BlockSpec(memory_space=pl.ANY)] * 6,
        out_specs=pl.BlockSpec(memory_space=pltpu.VMEM),
        scratch_shapes=[
            pltpu.VMEM((2, rows, width), BF16),
            pltpu.VMEM((count, 3, 2, cells, cells), BF16),
            pltpu.VMEM((count, 6 * cells, cells), BF16),
            pltpu.VMEM((2, 2, rank, width), BF16),
            pltpu.VMEM((2, 2, rank, width), BF16),
            pltpu.VMEM((2, 2, rank, width), BF16),
            pltpu.VMEM((4 * rank, width), BF16),
            pltpu.VMEM(coupling.shape, BF16),
            pltpu.SMEM(ranks.shape, jnp.int32),
            pltpu.VMEM((2, rows, width), F32),
            pltpu.VMEM((count, 2 * group, cells), F32),
            pltpu.VMEM((2, 2, rows, cells), BF16),
            pltpu.VMEM((sources,) + fold_shape(rows), BF16),
            pltpu.VMEM((2,) + fold_shape(rows), BF16),
            pltpu.VMEM((batches, 2, group, width), BF16),
            pltpu.VMEM((batches, 2, group, width), BF16),
            pltpu.VMEM((batches, 2, 2, group, cells), BF16),
            pltpu.VMEM((batches, sources) + fold_shape(group), BF16),
            pltpu.VMEM((batches, 2) + fold_shape(group), BF16),
            dma((6,)),
            dma((2, 2)),
            dma((2,)),
            dma((2, 2)),
            dma((batches, 2)),
            dma((batches, 2)),
            dma((2, batches)),
            dma((4,)),
            pltpu.SemaphoreType.REGULAR,
        ],
        compiler_params=pltpu.CompilerParams(collective_id=0, has_side_effects=True),
    )(right_side, near_blocks, right_bases, left_bases, coupling, ranks)


def solution(mesh):
    placed = (
        P("layer", None, None, "leaf"),
        P("layer", None, None, "leaf", None),
        P("layer", None, None, None, "leaf"),
        P("layer", None, None, None, "leaf"),
        P("layer", "leaf"),
        P("layer", None),
    )
    return jax.shard_map(
        functools.partial(body, mesh.shape["layer"], mesh.shape["leaf"]),
        mesh=mesh, in_specs=placed, out_specs=P("layer", None, None, "leaf"), check_vma=False,
    )
```

```python
import functools

import jax
import jax.numpy as jnp
from jax import lax
from jax.experimental import pallas as pl
from jax.experimental.pallas import tpu as pltpu
from jax.sharding import PartitionSpec as P

BATCHES = 4
TILE = 128
F32 = jnp.float32
BF16 = jnp.bfloat16
LANES = (((1,), (1,)), ((), ()))


def kernel(
    layers, leafs, batches,
    source_hbm, near_hbm, right_hbm, left_hbm, coupling_hbm, ranks_hbm,
    out_ref,
    source, near, near_turned, right, right_next, left_raw, left, coupling_ref, ranks_ref,
    inner, base, rim, part, part_sent, moved, sent, moved_rim, moved_part, moved_part_sent,
    load_sem, rim_sem, part_sem, right_sem, move_sem, move_rim_sem, move_part_sem, sent_sem, ready_sem,
):
    layer = lax.axis_index("layer")
    leaf = lax.axis_index("leaf")
    rows, width = source.shape[1], source.shape[2]
    cells = near.shape[-1]
    count = width // cells
    rank = right.shape[2]
    group = rows // batches
    half, quarter = leafs // 2, leafs // 4
    upper, lower = leaf // half, leaf // quarter
    has_low, has_high = leaf > 0, leaf < leafs - 1
    odd, even = lax.rem(leaf, 2) == 1, lax.rem(leaf, 2) == 0
    has_prev, has_next = layer > 0, layer < layers - 1
    edges = [0, count - 1] if count > 1 else [0]

    def remote(src, dst, sems, index, to_layer, to_leaf):
        return pltpu.make_async_remote_copy(
            src_ref=src, dst_ref=dst,
            send_sem=sems.at[(0,) + index],
            recv_sem=sems.at[(1,) + index],
            device_id=(to_layer, to_leaf), device_id_type=pl.DeviceIdType.MESH,
        )

    barrier = pltpu.get_barrier_semaphore()

    def greet(to_layer, to_leaf):
        pl.semaphore_signal(
            barrier, inc=1, device_id=(to_layer, to_leaf), device_id_type=pl.DeviceIdType.MESH
        )

    for step in range(1, leafs):
        greet(layer, lax.rem(leaf + step, leafs))

    pl.when(has_prev)(lambda: greet(layer - 1, leaf))
    pl.when(has_next)(lambda: greet(layer + 1, leaf))

    loads = [
        pltpu.make_async_copy(source_hbm.at[0], source, load_sem.at[0]),
        pltpu.make_async_copy(right_hbm.at[0], right, load_sem.at[1]),
        pltpu.make_async_copy(left_hbm.at[0], left_raw, load_sem.at[2]),
        pltpu.make_async_copy(coupling_hbm, coupling_ref, load_sem.at[3]),
        pltpu.make_async_copy(ranks_hbm, ranks_ref, load_sem.at[4]),
    ]
    near_loads = [
        pltpu.make_async_copy(
            near_hbm.at[0, :, :, pl.ds(q * cells, cells), :], near.at[q], load_sem.at[5]
        )
        for q in range(count)
    ]
    for copy in loads + near_loads:
        copy.start()

    @pl.when(jnp.logical_not(has_low))
    def _():
        rim[0] = jnp.zeros(rim.shape[1:], BF16)
        for b in range(batches):
            moved_rim[b, 0] = jnp.zeros(moved_rim.shape[2:], BF16)

    @pl.when(jnp.logical_not(has_high))
    def _():
        rim[1] = jnp.zeros(rim.shape[1:], BF16)
        for b in range(batches):
            moved_rim[b, 1] = jnp.zeros(moved_rim.shape[2:], BF16)

    def block(q):
        return pl.ds(q * cells, cells)

    def stacked(real, imag):
        return jnp.concatenate(
            [
                jnp.concatenate([real, imag], axis=0),
                jnp.concatenate([-imag, real], axis=0),
            ],
            axis=1,
        )

    def piece(field, q):
        return stacked(field[0, :, block(q)], field[1, :, block(q)])

    def sides(q):
        return [0] + ([1] if q > 0 else []) + ([2] if q < count - 1 else [])

    def shifted(q, s):
        return q + (0, -1, 1)[s]

    def level_sums(pieces, bases):
        flat = [bases[c, :, block(q)] for q in range(count) for c in range(2)]
        return lax.dot_general(
            jnp.concatenate(pieces, axis=1), jnp.concatenate(flat, axis=1), LANES,
            preferred_element_type=F32,
        )

    def folded(pieces, bases):
        flat = [
            bases[:, c, :, block(q)].reshape(2 * rank, cells) for q in range(count) for c in range(2)
        ]
        total = lax.dot_general(
            jnp.concatenate(pieces, axis=1), jnp.concatenate(flat, axis=1), LANES,
            preferred_element_type=F32,
        )
        return [packed(total[:, level * rank:(level + 1) * rank]) for level in range(2)]

    def packed(total):
        height = max(total.shape[0] * total.shape[1] // TILE, 1)
        return jnp.concatenate(
            [total[at:at + height] for at in range(0, total.shape[0], height)], axis=1
        ).astype(BF16)

    def part_copies(src, dst, send_sem, recv_sem, to_layer):
        copies = []

        def part_copy(level, slot, to_leaf):
            return pltpu.make_async_remote_copy(
                src_ref=src.at[level], dst_ref=dst.at[slot], send_sem=send_sem, recv_sem=recv_sem,
                device_id=(to_layer, to_leaf), device_id_type=pl.DeviceIdType.MESH,
            )

        slot = lax.rem(leaf, half)
        for other in range(half):
            copies.append(part_copy(0, slot, (1 - upper) * half + other))
        slot = half + lax.rem(leaf, quarter)
        sibling = lower + 1 - 2 * lax.rem(lower, 2)
        for other in range(quarter):
            copies.append(part_copy(1, slot, sibling * quarter + other))
        return copies

    def landed(view, sem):
        pltpu.make_async_copy(view, view, sem).wait()

    def coefficients(parts):
        first = parts[0].astype(F32)
        for slot in range(1, half):
            first = first + parts[slot].astype(F32)
        second = parts[half].astype(F32)
        for slot in range(1, quarter):
            second = second + parts[half + slot].astype(F32)
        def unpacked(flat):
            return jnp.concatenate(
                [flat[:, at:at + rank] for at in range(0, flat.shape[1], rank)], axis=0
            )

        turned = jnp.concatenate([unpacked(first), unpacked(second)], axis=1)
        size = turned.shape[0] // 2
        swapped = jnp.concatenate([-turned[size:], turned[:size]], axis=0)
        return jnp.concatenate([turned, swapped], axis=1).astype(BF16)

    def far_leaf(q, coeff):
        return jnp.dot(coeff, left[:, block(q)], preferred_element_type=F32)

    def plain_dot(q, s, value):
        rhs = jnp.concatenate([near[q, s, 0], near[q, s, 1]], axis=1)
        return lax.dot_general(value, rhs, LANES, preferred_element_type=F32)

    def turned_dot(q, chosen, values):
        rhs = [near_turned[q, pl.ds(s * 2 * cells, 2 * cells), :] for s in chosen]
        return jnp.dot(
            jnp.concatenate(values, axis=1), jnp.concatenate(rhs, axis=0),
            preferred_element_type=F32,
        )

    loads[0].wait()
    loads[1].wait()
    source_pieces = [piece(source, q) for q in range(count)]
    part_sent[0], part_sent[1] = folded(source_pieces, right)

    pl.semaphore_wait(
        barrier, leafs - 1 + has_prev.astype(jnp.int32) + has_next.astype(jnp.int32)
    )

    downs = [
        remote(right.at[level], right_next.at[level], right_sem, (level,), layer - 1, leaf)
        for level in range(2)
    ]

    @pl.when(has_prev)
    def _():
        for copy in downs:
            copy.start()

    to_high = remote(
        source.at[:, :, block(count - 1)], rim.at[0], rim_sem, (0,), layer, leaf + 1
    )
    to_low = remote(source.at[:, :, block(0)], rim.at[1], rim_sem, (1,), layer, leaf - 1)
    source_parts = part_copies(part_sent, part, part_sem.at[0], part_sem.at[1], layer)

    @pl.when(has_prev)
    def _():
        pl.semaphore_signal(
            ready_sem, inc=1, device_id=(layer - 1, leaf), device_id_type=pl.DeviceIdType.MESH
        )

    for copy in source_parts:
        copy.start()
    pl.when(has_high)(to_high.start)
    pl.when(has_low)(to_low.start)

    loads[2].wait()
    loads[3].wait()
    loads[4].wait()
    row_ids = lax.broadcasted_iota(jnp.int32, (rank, width), 0)
    for level, slot in ((0, upper), (1, 2 + lower)):
        keep = (row_ids < ranks_ref[0, slot]).astype(F32)
        for c in range(2):
            left[pl.ds((2 * c + level) * rank, rank), :] = (
                left_raw[level, c].astype(F32) * keep
            ).astype(BF16)

    pltpu.make_async_copy(near, near, load_sem.at[5]).wait()
    for q in range(count):
        value = None
        for s in sides(q):
            term = plain_dot(q, s, source_pieces[shifted(q, s)])
            value = term if value is None else value + term
        inner[:, :, block(q)] = value.reshape(2, rows, cells)
    pl.when(has_low)(to_high.wait_recv)
    pl.when(has_high)(to_low.wait_recv)
    for q, s, side in ((0, 1, 0), (count - 1, 2, 1)):
        inner[:, :, block(q)] += plain_dot(q, s, stacked(rim[side, 0], rim[side, 1])).reshape(
            2, rows, cells
        )
    landed(part, part_sem.at[1])
    coeff = coefficients(part)
    for q in range(count):
        inner[:, :, block(q)] += far_leaf(q, coeff).reshape(2, rows, cells)

    @pl.when(has_prev)
    def _():
        for q in range(count):
            for s in range(3):
                for c in range(2):
                    near_turned[q, pl.ds((2 * s + c) * cells, cells), :] = near[q, s, c].T

    pl.when(has_next)(lambda: pl.semaphore_wait(ready_sem, 1))

    def rows_of(b):
        return pl.ds(b * group, group)

    def ahead_main(b):
        pairs = [(block(q), 0) for q in edges]
        if count > 2:
            pairs.append((pl.ds(cells, width - 2 * cells), 1))
        return [
            pltpu.make_async_remote_copy(
                src_ref=sent.at[b, :, :, span], dst_ref=moved.at[b, :, :, span],
                send_sem=sent_sem.at[0], recv_sem=move_sem.at[b, kind],
                device_id=(layer + 1, leaf), device_id_type=pl.DeviceIdType.MESH,
            )
            for span, kind in pairs
        ]

    def rim_copy(source_ref, q, b, side, to_layer, to_leaf):
        return pltpu.make_async_remote_copy(
            src_ref=source_ref.at[b, :, :, block(q)], dst_ref=moved_rim.at[b, side],
            send_sem=sent_sem.at[1 + side], recv_sem=move_rim_sem.at[b],
            device_id=(to_layer, to_leaf), device_id_type=pl.DeviceIdType.MESH,
        )

    def ahead_high(b):
        return rim_copy(sent, count - 1, b, 0, layer + 1, leaf + 1)

    def ahead_low(b):
        return rim_copy(sent, 0, b, 1, layer + 1, leaf - 1)

    def across_low(b):
        return pltpu.make_async_remote_copy(
            src_ref=moved.at[b, :, :, block(0)], dst_ref=moved_rim.at[b, 1],
            send_sem=sent_sem.at[3], recv_sem=move_rim_sem.at[b],
            device_id=(layer, leaf - 1), device_id_type=pl.DeviceIdType.MESH,
        )

    def hand_across(b):
        if b < batches:

            @pl.when(odd)
            def _():
                wait_edges(b)
                across_low(b).start()

    def ahead_parts(b):
        return part_copies(
            moved_part_sent.at[b], moved_part.at[b], sent_sem.at[4], move_part_sem.at[b], layer + 1
        )


    def wait_edges(b):
        view = moved.at[b, :, :, pl.ds(0, len(edges) * cells)]
        pltpu.make_async_copy(view, view, move_sem.at[b, 0]).wait()

    def wait_middle(b):
        if count > 2:
            view = moved.at[b, :, :, pl.ds(cells, width - 2 * cells)]
            pltpu.make_async_copy(view, view, move_sem.at[b, 1]).wait()

    def wait_rims(b):
        sem = move_rim_sem.at[b]
        pl.when(has_low & has_high)(lambda: landed(moved_rim.at[b], sem))
        pl.when(jnp.logical_not(has_high))(lambda: landed(moved_rim.at[b, 0], sem))
        pl.when(jnp.logical_not(has_low))(lambda: landed(moved_rim.at[b, 1], sem))

    def receive_whole(b):
        pl.when(even)(lambda: wait_edges(b))
        wait_middle(b)
        wait_rims(b)
        landed(moved_part.at[b], move_part_sem.at[b])
        hand_across(b + 1)
        coeff = coefficients(moved_part[b])
        pieces = [stacked(moved_rim[b, 0, 0], moved_rim[b, 0, 1])]
        pieces += [piece(moved.at[b], q) for q in range(count)]
        pieces += [stacked(moved_rim[b, 1, 0], moved_rim[b, 1, 1])]
        fields = []
        for q in range(count):
            lhs = jnp.concatenate([pieces[q + 1], pieces[q], pieces[q + 2], coeff], axis=1)
            rhs = jnp.concatenate([near_turned[q], left[:, block(q)]], axis=0)
            value = inner[:, rows_of(b), block(q)].reshape(2 * group, cells) - jnp.dot(
                lhs, rhs, preferred_element_type=F32
            )
            swept = value.astype(BF16).reshape(2, group, cells)
            out_ref[0, :, rows_of(b), block(q)] = swept
            fields.append(swept)
        return fields

    def receive(b, staged):
        if not staged:
            return receive_whole(b)
        def gathered(q, chosen):
            return turned_dot(q, chosen, [pieces[shifted(q, s)] for s in chosen])

        hand_across(b)
        pl.when(even)(lambda: wait_edges(b))
        pieces = {q: piece(moved.at[b], q) for q in edges}
        left_over = {}
        for q in range(count):
            value = inner[:, rows_of(b), block(q)].reshape(2 * group, cells)
            chosen = [s for s in sides(q) if shifted(q, s) in pieces]
            left_over[q] = [s for s in sides(q) if s not in chosen]
            base[q] = value - gathered(q, chosen) if chosen else value
        wait_middle(b)
        pieces.update({q: piece(moved.at[b], q) for q in range(1, count - 1)})
        for q in range(count):
            if left_over[q]:
                base[q] -= gathered(q, left_over[q])
        wait_rims(b)
        hand_across(b + 1)
        landed(moved_part.at[b], move_part_sem.at[b])
        coeff = coefficients(moved_part[b])
        fields = []
        for q in range(count):
            values, weights = [coeff], [left[:, block(q)]]
            for at, s, side in ((0, 1, 0), (count - 1, 2, 1)):
                if at == q:
                    values.append(stacked(moved_rim[b, side, 0], moved_rim[b, side, 1]))
                    weights.append(near_turned[q, pl.ds(s * 2 * cells, 2 * cells), :])
            value = base[q]
            for one, weight in zip(values, weights):
                value = value - jnp.dot(one, weight, preferred_element_type=F32)
            swept = value.astype(BF16).reshape(2, group, cells)
            out_ref[0, :, rows_of(b), block(q)] = swept
            fields.append(swept)
        return fields

    def couple(b, fields):
        coupled = []
        for q in range(count):
            value = (coupling_ref[:, block(q)].astype(F32)[None] * fields[q].astype(F32)).astype(BF16)
            sent[b, :, :, block(q)] = value
            coupled.append(stacked(value[0], value[1]))
        return coupled

    def send_rims(b):
        pl.when(has_high)(ahead_high(b).start)
        pl.when(even & has_low)(ahead_low(b).start)

    def send_main(b):
        for copy in ahead_main(b):
            copy.start()

    def send_field(b):
        send_rims(b)
        send_main(b)

    def send_parts(b, stacks):
        moved_part_sent[b, 0], moved_part_sent[b, 1] = folded(stacks, right_next)
        for copy in ahead_parts(b):
            copy.start()

    def emit_first():
        for b in range(batches):
            couple(b, [out_ref[0, :, rows_of(b), block(q)] for q in range(count)])
            if b == 0:
                send_field(b)
        stacks = [piece(sent.at[0], q) for q in range(count)]
        downs[0].wait_recv()
        moved_part_sent[0, 0] = packed(level_sums(stacks, right_next.at[0]))
        for copy in ahead_parts(0)[:half]:
            copy.start()
        if batches > 1:
            for copy in ahead_main(1)[:len(edges)]:
                copy.start()
        downs[1].wait_recv()
        moved_part_sent[0, 1] = packed(level_sums(stacks, right_next.at[1]))
        for copy in ahead_parts(0)[half:]:
            copy.start()
        if batches > 1:
            for copy in ahead_main(1)[len(edges):]:
                copy.start()
            send_rims(1)
        for b in range(1, batches):
            send_parts(b, [piece(sent.at[b], q) for q in range(count)])
            if b > 1:
                send_field(b)

    @pl.when(jnp.logical_not(has_prev))
    def _():
        out_ref[0] = inner[...].astype(BF16)
        pl.when(has_next)(emit_first)

    @pl.when(has_prev & has_next)
    def _():
        for b in range(batches):
            if b == 0:
                for copy in downs:
                    copy.wait_recv()
            stacks = couple(b, receive(b, b == 0))
            send_rims(b)
            send_parts(b, stacks)
            send_main(b)

    @pl.when(has_prev & jnp.logical_not(has_next))
    def _():
        for b in range(batches):
            receive(b, b == 0)

    pl.when(has_high)(to_high.wait_send)
    pl.when(has_low)(to_low.wait_send)
    landed(part, part_sem.at[0])

    @pl.when(has_prev)
    def _():
        for copy in downs:
            copy.wait_send()


    def drained(ref, index):
        pltpu.make_async_copy(ref, ref, sent_sem.at[index]).wait()

    pl.when(has_prev & odd)(lambda: drained(moved_rim.at[:, 1], 3))

    @pl.when(has_next)
    def _():
        drained(sent, 0)
        pl.when(has_high)(lambda: drained(moved_rim.at[:, 0], 1))
        pl.when(even & has_low)(lambda: drained(moved_rim.at[:, 1], 2))
        drained(moved_part, 4)


def body(layers, leafs, right_side, near_blocks, right_bases, left_bases, coupling, ranks):
    rows, width = right_side.shape[2:]
    cells = near_blocks.shape[-1]
    rank = right_bases.shape[3]
    count = width // cells
    batches = BATCHES
    group = rows // batches
    sources = leafs // 2 + leafs // 4
    dma = pltpu.SemaphoreType.DMA

    def fold_shape(size):
        height = max(2 * size * rank // TILE, 1)
        return (height, 2 * size * rank // height)

    return pl.pallas_call(
        functools.partial(kernel, layers, leafs, batches),
        out_shape=pltpu.VMEM(right_side.shape, BF16),
        in_specs=[pl.BlockSpec(memory_space=pl.ANY)] * 6,
        out_specs=pl.BlockSpec(memory_space=pltpu.VMEM),
        scratch_shapes=[
            pltpu.VMEM((2, rows, width), BF16),
            pltpu.VMEM((count, 3, 2, cells, cells), BF16),
            pltpu.VMEM((count, 6 * cells, cells), BF16),
            pltpu.VMEM((2, 2, rank, width), BF16),
            pltpu.VMEM((2, 2, rank, width), BF16),
            pltpu.VMEM((2, 2, rank, width), BF16),
            pltpu.VMEM((4 * rank, width), BF16),
            pltpu.VMEM(coupling.shape, BF16),
            pltpu.SMEM(ranks.shape, jnp.int32),
            pltpu.VMEM((2, rows, width), F32),
            pltpu.VMEM((count, 2 * group, cells), F32),
            pltpu.VMEM((2, 2, rows, cells), BF16),
            pltpu.VMEM((sources,) + fold_shape(rows), BF16),
            pltpu.VMEM((2,) + fold_shape(rows), BF16),
            pltpu.VMEM((batches, 2, group, width), BF16),
            pltpu.VMEM((batches, 2, group, width), BF16),
            pltpu.VMEM((batches, 2, 2, group, cells), BF16),
            pltpu.VMEM((batches, sources) + fold_shape(group), BF16),
            pltpu.VMEM((batches, 2) + fold_shape(group), BF16),
            dma((6,)),
            dma((2, 2)),
            dma((2,)),
            dma((2, 2)),
            dma((batches, 2)),
            dma((batches,)),
            dma((batches,)),
            dma((5,)),
            pltpu.SemaphoreType.REGULAR,
        ],
        compiler_params=pltpu.CompilerParams(collective_id=0, has_side_effects=True),
    )(right_side, near_blocks, right_bases, left_bases, coupling, ranks)


def solution(mesh):
    placed = (
        P("layer", None, None, "leaf"),
        P("layer", None, None, "leaf", None),
        P("layer", None, None, None, "leaf"),
        P("layer", None, None, None, "leaf"),
        P("layer", "leaf"),
        P("layer", None),
    )
    return jax.shard_map(
        functools.partial(body, mesh.shape["layer"], mesh.shape["leaf"]),
        mesh=mesh, in_specs=placed, out_specs=P("layer", None, None, "leaf"), check_vma=False,
    )
```

```python
import functools

import jax
import jax.numpy as jnp
from jax import lax
from jax.experimental import pallas as pl
from jax.experimental.pallas import tpu as pltpu
from jax.sharding import PartitionSpec as P

BATCHES = 4
TILE = 128
F32 = jnp.float32
BF16 = jnp.bfloat16
LANES = (((1,), (1,)), ((), ()))


def kernel(
    layers, leafs, batches,
    source_hbm, near_hbm, right_hbm, left_hbm, coupling_hbm, ranks_hbm,
    out_ref,
    source, near, near_turned, right, right_next, left_raw, left, coupling_ref, ranks_ref,
    inner, base, rim, part, part_sent, moved, sent, moved_rim, moved_part, moved_part_sent,
    load_sem, rim_sem, part_sem, right_sem, move_sem, move_rim_sem, move_part_sem, sent_sem, ready_sem,
):
    layer = lax.axis_index("layer")
    leaf = lax.axis_index("leaf")
    rows, width = source.shape[1], source.shape[2]
    cells = near.shape[-1]
    count = width // cells
    rank = right.shape[2]
    group = rows // batches
    half, quarter = leafs // 2, leafs // 4
    upper, lower = leaf // half, leaf // quarter
    has_low, has_high = leaf > 0, leaf < leafs - 1
    odd, even = lax.rem(leaf, 2) == 1, lax.rem(leaf, 2) == 0
    has_prev, has_next = layer > 0, layer < layers - 1
    edges = [0, count - 1] if count > 1 else [0]

    def remote(src, dst, sems, index, to_layer, to_leaf):
        return pltpu.make_async_remote_copy(
            src_ref=src, dst_ref=dst,
            send_sem=sems.at[(0,) + index],
            recv_sem=sems.at[(1,) + index],
            device_id=(to_layer, to_leaf), device_id_type=pl.DeviceIdType.MESH,
        )

    barrier = pltpu.get_barrier_semaphore()

    def greet(to_layer, to_leaf):
        pl.semaphore_signal(
            barrier, inc=1, device_id=(to_layer, to_leaf), device_id_type=pl.DeviceIdType.MESH
        )

    for step in range(1, leafs):
        greet(layer, lax.rem(leaf + step, leafs))

    pl.when(has_prev)(lambda: greet(layer - 1, leaf))
    pl.when(has_next)(lambda: greet(layer + 1, leaf))

    loads = [
        pltpu.make_async_copy(source_hbm.at[0], source, load_sem.at[0]),
        pltpu.make_async_copy(right_hbm.at[0], right, load_sem.at[1]),
        pltpu.make_async_copy(left_hbm.at[0], left_raw, load_sem.at[2]),
        pltpu.make_async_copy(coupling_hbm, coupling_ref, load_sem.at[3]),
        pltpu.make_async_copy(ranks_hbm, ranks_ref, load_sem.at[4]),
    ]
    near_loads = [
        pltpu.make_async_copy(
            near_hbm.at[0, :, :, pl.ds(q * cells, cells), :], near.at[q], load_sem.at[5]
        )
        for q in range(count)
    ]
    for copy in loads + near_loads:
        copy.start()

    @pl.when(jnp.logical_not(has_low))
    def _():
        rim[0] = jnp.zeros(rim.shape[1:], BF16)
        for b in range(batches):
            moved_rim[b, 0] = jnp.zeros(moved_rim.shape[2:], BF16)

    @pl.when(jnp.logical_not(has_high))
    def _():
        rim[1] = jnp.zeros(rim.shape[1:], BF16)
        for b in range(batches):
            moved_rim[b, 1] = jnp.zeros(moved_rim.shape[2:], BF16)

    def block(q):
        return pl.ds(q * cells, cells)

    def stacked(real, imag):
        return jnp.concatenate(
            [
                jnp.concatenate([real, imag], axis=0),
                jnp.concatenate([-imag, real], axis=0),
            ],
            axis=1,
        )

    def piece(field, q):
        return stacked(field[0, :, block(q)], field[1, :, block(q)])

    def sides(q):
        return [0] + ([1] if q > 0 else []) + ([2] if q < count - 1 else [])

    def shifted(q, s):
        return q + (0, -1, 1)[s]

    def level_sums(pieces, bases):
        flat = [bases[c, :, block(q)] for q in range(count) for c in range(2)]
        return lax.dot_general(
            jnp.concatenate(pieces, axis=1), jnp.concatenate(flat, axis=1), LANES,
            preferred_element_type=F32,
        )

    def folded(pieces, bases):
        flat = [
            bases[:, c, :, block(q)].reshape(2 * rank, cells) for q in range(count) for c in range(2)
        ]
        total = lax.dot_general(
            jnp.concatenate(pieces, axis=1), jnp.concatenate(flat, axis=1), LANES,
            preferred_element_type=F32,
        )
        return [packed(total[:, level * rank:(level + 1) * rank]) for level in range(2)]

    def packed(total):
        height = max(total.shape[0] * total.shape[1] // TILE, 1)
        return jnp.concatenate(
            [total[at:at + height] for at in range(0, total.shape[0], height)], axis=1
        ).astype(BF16)

    def part_copies(src, dst, send_sem, recv_sem, to_layer):
        copies = []

        def part_copy(level, slot, to_leaf):
            return pltpu.make_async_remote_copy(
                src_ref=src.at[level], dst_ref=dst.at[slot], send_sem=send_sem, recv_sem=recv_sem,
                device_id=(to_layer, to_leaf), device_id_type=pl.DeviceIdType.MESH,
            )

        slot = lax.rem(leaf, half)
        for other in range(half):
            copies.append(part_copy(0, slot, (1 - upper) * half + other))
        slot = half + lax.rem(leaf, quarter)
        sibling = lower + 1 - 2 * lax.rem(lower, 2)
        for other in range(quarter):
            copies.append(part_copy(1, slot, sibling * quarter + other))
        return copies

    def landed(view, sem):
        pltpu.make_async_copy(view, view, sem).wait()

    def coefficients(parts):
        first = parts[0].astype(F32)
        for slot in range(1, half):
            first = first + parts[slot].astype(F32)
        second = parts[half].astype(F32)
        for slot in range(1, quarter):
            second = second + parts[half + slot].astype(F32)
        def unpacked(flat):
            return jnp.concatenate(
                [flat[:, at:at + rank] for at in range(0, flat.shape[1], rank)], axis=0
            )

        turned = jnp.concatenate([unpacked(first), unpacked(second)], axis=1)
        size = turned.shape[0] // 2
        swapped = jnp.concatenate([-turned[size:], turned[:size]], axis=0)
        return jnp.concatenate([turned, swapped], axis=1).astype(BF16)

    def far_leaf(q, coeff):
        return jnp.dot(coeff, left[:, block(q)], preferred_element_type=F32)

    def plain_dot(q, s, value):
        rhs = jnp.concatenate([near[q, s, 0], near[q, s, 1]], axis=1)
        return lax.dot_general(value, rhs, LANES, preferred_element_type=F32)

    def turned_dot(q, chosen, values):
        rhs = [near_turned[q, pl.ds(s * 2 * cells, 2 * cells), :] for s in chosen]
        return jnp.dot(
            jnp.concatenate(values, axis=1), jnp.concatenate(rhs, axis=0),
            preferred_element_type=F32,
        )

    loads[0].wait()
    loads[1].wait()
    source_pieces = [piece(source, q) for q in range(count)]
    part_sent[0], part_sent[1] = folded(source_pieces, right)

    pl.semaphore_wait(
        barrier, leafs - 1 + has_prev.astype(jnp.int32) + has_next.astype(jnp.int32)
    )

    downs = [
        remote(right.at[level], right_next.at[level], right_sem, (level,), layer - 1, leaf)
        for level in range(2)
    ]

    @pl.when(has_prev)
    def _():
        for copy in downs:
            copy.start()

    to_high = remote(
        source.at[:, :, block(count - 1)], rim.at[0], rim_sem, (0,), layer, leaf + 1
    )
    to_low = remote(source.at[:, :, block(0)], rim.at[1], rim_sem, (1,), layer, leaf - 1)
    source_parts = part_copies(part_sent, part, part_sem.at[0], part_sem.at[1], layer)

    @pl.when(has_prev)
    def _():
        pl.semaphore_signal(
            ready_sem, inc=1, device_id=(layer - 1, leaf), device_id_type=pl.DeviceIdType.MESH
        )

    for copy in source_parts:
        copy.start()
    pl.when(has_high)(to_high.start)
    pl.when(has_low)(to_low.start)

    loads[2].wait()
    loads[3].wait()
    loads[4].wait()
    row_ids = lax.broadcasted_iota(jnp.int32, (rank, width), 0)
    for level, slot in ((0, upper), (1, 2 + lower)):
        keep = (row_ids < ranks_ref[0, slot]).astype(F32)
        for c in range(2):
            left[pl.ds((2 * c + level) * rank, rank), :] = (
                left_raw[level, c].astype(F32) * keep
            ).astype(BF16)

    pltpu.make_async_copy(near, near, load_sem.at[5]).wait()
    for q in range(count):
        value = None
        for s in sides(q):
            term = plain_dot(q, s, source_pieces[shifted(q, s)])
            value = term if value is None else value + term
        inner[:, :, block(q)] = value.reshape(2, rows, cells)
    pl.when(has_low)(to_high.wait_recv)
    pl.when(has_high)(to_low.wait_recv)
    for q, s, side in ((0, 1, 0), (count - 1, 2, 1)):
        inner[:, :, block(q)] += plain_dot(q, s, stacked(rim[side, 0], rim[side, 1])).reshape(
            2, rows, cells
        )
    landed(part, part_sem.at[1])
    coeff = coefficients(part)
    for q in range(count):
        inner[:, :, block(q)] += far_leaf(q, coeff).reshape(2, rows, cells)

    @pl.when(has_prev)
    def _():
        for q in range(count):
            for s in range(3):
                for c in range(2):
                    near_turned[q, pl.ds((2 * s + c) * cells, cells), :] = near[q, s, c].T

    pl.when(has_next)(lambda: pl.semaphore_wait(ready_sem, 1))

    pl.when(has_high)(to_high.wait_send)
    pl.when(has_low)(to_low.wait_send)
    landed(part, part_sem.at[0])

    @pl.when(has_prev)
    def _():
        for copy in downs:
            copy.wait_send()

    def rows_of(b):
        return pl.ds(b * group, group)

    def ahead_main(b):
        pairs = [(block(q), 0) for q in edges]
        if count > 2:
            pairs.append((pl.ds(cells, width - 2 * cells), 1))
        return [
            pltpu.make_async_remote_copy(
                src_ref=sent.at[b, :, :, span], dst_ref=moved.at[b, :, :, span],
                send_sem=sent_sem.at[0], recv_sem=move_sem.at[b, kind],
                device_id=(layer + 1, leaf), device_id_type=pl.DeviceIdType.MESH,
            )
            for span, kind in pairs
        ]

    def rim_copy(source_ref, q, b, side, to_layer, to_leaf):
        return pltpu.make_async_remote_copy(
            src_ref=source_ref.at[b, :, :, block(q)], dst_ref=moved_rim.at[b, side],
            send_sem=sent_sem.at[1 + side], recv_sem=move_rim_sem.at[b],
            device_id=(to_layer, to_leaf), device_id_type=pl.DeviceIdType.MESH,
        )

    def ahead_high(b):
        return rim_copy(sent, count - 1, b, 0, layer + 1, leaf + 1)

    def ahead_low(b):
        return rim_copy(sent, 0, b, 1, layer + 1, leaf - 1)

    def across_low(b):
        return pltpu.make_async_remote_copy(
            src_ref=moved.at[b, :, :, block(0)], dst_ref=moved_rim.at[b, 1],
            send_sem=sent_sem.at[3], recv_sem=move_rim_sem.at[b],
            device_id=(layer, leaf - 1), device_id_type=pl.DeviceIdType.MESH,
        )

    def hand_across(b):
        if b < batches:

            @pl.when(odd)
            def _():
                wait_edges(b)
                across_low(b).start()

    def ahead_parts(b):
        return part_copies(
            moved_part_sent.at[b], moved_part.at[b], sent_sem.at[4], move_part_sem.at[b], layer + 1
        )


    def wait_edges(b):
        view = moved.at[b, :, :, pl.ds(0, len(edges) * cells)]
        pltpu.make_async_copy(view, view, move_sem.at[b, 0]).wait()

    def wait_middle(b):
        if count > 2:
            view = moved.at[b, :, :, pl.ds(cells, width - 2 * cells)]
            pltpu.make_async_copy(view, view, move_sem.at[b, 1]).wait()

    def wait_rims(b):
        sem = move_rim_sem.at[b]
        pl.when(has_low & has_high)(lambda: landed(moved_rim.at[b], sem))
        pl.when(jnp.logical_not(has_high))(lambda: landed(moved_rim.at[b, 0], sem))
        pl.when(jnp.logical_not(has_low))(lambda: landed(moved_rim.at[b, 1], sem))

    def receive_whole(b):
        pl.when(even)(lambda: wait_edges(b))
        wait_middle(b)
        wait_rims(b)
        landed(moved_part.at[b], move_part_sem.at[b])
        hand_across(b + 1)
        coeff = coefficients(moved_part[b])
        pieces = [stacked(moved_rim[b, 0, 0], moved_rim[b, 0, 1])]
        pieces += [piece(moved.at[b], q) for q in range(count)]
        pieces += [stacked(moved_rim[b, 1, 0], moved_rim[b, 1, 1])]
        fields = []
        for q in range(count):
            lhs = jnp.concatenate([pieces[q + 1], pieces[q], pieces[q + 2], coeff], axis=1)
            rhs = jnp.concatenate([near_turned[q], left[:, block(q)]], axis=0)
            value = inner[:, rows_of(b), block(q)].reshape(2 * group, cells) - jnp.dot(
                lhs, rhs, preferred_element_type=F32
            )
            swept = value.astype(BF16).reshape(2, group, cells)
            out_ref[0, :, rows_of(b), block(q)] = swept
            fields.append(swept)
        return fields

    def receive(b, staged):
        if not staged:
            return receive_whole(b)
        def gathered(q, chosen):
            return turned_dot(q, chosen, [pieces[shifted(q, s)] for s in chosen])

        hand_across(b)
        pl.when(even)(lambda: wait_edges(b))
        pieces = {q: piece(moved.at[b], q) for q in edges}
        left_over = {}
        for q in range(count):
            value = inner[:, rows_of(b), block(q)].reshape(2 * group, cells)
            chosen = [s for s in sides(q) if shifted(q, s) in pieces]
            left_over[q] = [s for s in sides(q) if s not in chosen]
            base[q] = value - gathered(q, chosen) if chosen else value
        wait_middle(b)
        pieces.update({q: piece(moved.at[b], q) for q in range(1, count - 1)})
        for q in range(count):
            if left_over[q]:
                base[q] -= gathered(q, left_over[q])
        wait_rims(b)
        hand_across(b + 1)
        landed(moved_part.at[b], move_part_sem.at[b])
        coeff = coefficients(moved_part[b])
        fields = []
        for q in range(count):
            values, weights = [coeff], [left[:, block(q)]]
            for at, s, side in ((0, 1, 0), (count - 1, 2, 1)):
                if at == q:
                    values.append(stacked(moved_rim[b, side, 0], moved_rim[b, side, 1]))
                    weights.append(near_turned[q, pl.ds(s * 2 * cells, 2 * cells), :])
            value = base[q]
            for one, weight in zip(values, weights):
                value = value - jnp.dot(one, weight, preferred_element_type=F32)
            swept = value.astype(BF16).reshape(2, group, cells)
            out_ref[0, :, rows_of(b), block(q)] = swept
            fields.append(swept)
        return fields

    def couple(b, fields):
        coupled = []
        for q in range(count):
            value = (coupling_ref[:, block(q)].astype(F32)[None] * fields[q].astype(F32)).astype(BF16)
            sent[b, :, :, block(q)] = value
            coupled.append(stacked(value[0], value[1]))
        return coupled

    def send_rims(b):
        pl.when(has_high)(ahead_high(b).start)
        pl.when(even & has_low)(ahead_low(b).start)

    def send_main(b):
        for copy in ahead_main(b):
            copy.start()

    def send_field(b):
        send_rims(b)
        send_main(b)

    def send_parts(b, stacks):
        moved_part_sent[b, 0], moved_part_sent[b, 1] = folded(stacks, right_next)
        for copy in ahead_parts(b):
            copy.start()

    def emit_first():
        for b in range(batches):
            couple(b, [out_ref[0, :, rows_of(b), block(q)] for q in range(count)])
            if b == 0:
                send_field(b)
        stacks = [piece(sent.at[0], q) for q in range(count)]
        downs[0].wait_recv()
        moved_part_sent[0, 0] = packed(level_sums(stacks, right_next.at[0]))
        for copy in ahead_parts(0)[:half]:
            copy.start()
        if batches > 1:
            for copy in ahead_main(1)[:len(edges)]:
                copy.start()
        downs[1].wait_recv()
        moved_part_sent[0, 1] = packed(level_sums(stacks, right_next.at[1]))
        for copy in ahead_parts(0)[half:]:
            copy.start()
        if batches > 1:
            for copy in ahead_main(1)[len(edges):]:
                copy.start()
            send_rims(1)
        for b in range(1, batches):
            send_parts(b, [piece(sent.at[b], q) for q in range(count)])
            if b > 1:
                send_field(b)

    @pl.when(jnp.logical_not(has_prev))
    def _():
        out_ref[0] = inner[...].astype(BF16)
        pl.when(has_next)(emit_first)

    @pl.when(has_prev & has_next)
    def _():
        for b in range(batches):
            if b == 0:
                for copy in downs:
                    copy.wait_recv()
            stacks = couple(b, receive(b, b == 0))
            send_rims(b)
            send_parts(b, stacks)
            send_main(b)

    @pl.when(has_prev & jnp.logical_not(has_next))
    def _():
        for b in range(batches):
            receive(b, b == 0)

    def drained(ref, index):
        pltpu.make_async_copy(ref, ref, sent_sem.at[index]).wait()

    pl.when(has_prev & odd)(lambda: drained(moved_rim.at[:, 1], 3))

    @pl.when(has_next)
    def _():
        drained(sent, 0)
        pl.when(has_high)(lambda: drained(moved_rim.at[:, 0], 1))
        pl.when(even & has_low)(lambda: drained(moved_rim.at[:, 1], 2))
        drained(moved_part, 4)


def body(layers, leafs, right_side, near_blocks, right_bases, left_bases, coupling, ranks):
    rows, width = right_side.shape[2:]
    cells = near_blocks.shape[-1]
    rank = right_bases.shape[3]
    count = width // cells
    batches = BATCHES
    group = rows // batches
    sources = leafs // 2 + leafs // 4
    dma = pltpu.SemaphoreType.DMA

    def fold_shape(size):
        height = max(2 * size * rank // TILE, 1)
        return (height, 2 * size * rank // height)

    return pl.pallas_call(
        functools.partial(kernel, layers, leafs, batches),
        out_shape=pltpu.VMEM(right_side.shape, BF16),
        in_specs=[pl.BlockSpec(memory_space=pl.ANY)] * 6,
        out_specs=pl.BlockSpec(memory_space=pltpu.VMEM),
        scratch_shapes=[
            pltpu.VMEM((2, rows, width), BF16),
            pltpu.VMEM((count, 3, 2, cells, cells), BF16),
            pltpu.VMEM((count, 6 * cells, cells), BF16),
            pltpu.VMEM((2, 2, rank, width), BF16),
            pltpu.VMEM((2, 2, rank, width), BF16),
            pltpu.VMEM((2, 2, rank, width), BF16),
            pltpu.VMEM((4 * rank, width), BF16),
            pltpu.VMEM(coupling.shape, BF16),
            pltpu.SMEM(ranks.shape, jnp.int32),
            pltpu.VMEM((2, rows, width), F32),
            pltpu.VMEM((count, 2 * group, cells), F32),
            pltpu.VMEM((2, 2, rows, cells), BF16),
            pltpu.VMEM((sources,) + fold_shape(rows), BF16),
            pltpu.VMEM((2,) + fold_shape(rows), BF16),
            pltpu.VMEM((batches, 2, group, width), BF16),
            pltpu.VMEM((batches, 2, group, width), BF16),
            pltpu.VMEM((batches, 2, 2, group, cells), BF16),
            pltpu.VMEM((batches, sources) + fold_shape(group), BF16),
            pltpu.VMEM((batches, 2) + fold_shape(group), BF16),
            dma((6,)),
            dma((2, 2)),
            dma((2,)),
            dma((2, 2)),
            dma((batches, 2)),
            dma((batches,)),
            dma((batches,)),
            dma((5,)),
            pltpu.SemaphoreType.REGULAR,
        ],
        compiler_params=pltpu.CompilerParams(collective_id=0, has_side_effects=True),
    )(right_side, near_blocks, right_bases, left_bases, coupling, ranks)


def solution(mesh):
    placed = (
        P("layer", None, None, "leaf"),
        P("layer", None, None, "leaf", None),
        P("layer", None, None, None, "leaf"),
        P("layer", None, None, None, "leaf"),
        P("layer", "leaf"),
        P("layer", None),
    )
    return jax.shard_map(
        functools.partial(body, mesh.shape["layer"], mesh.shape["leaf"]),
        mesh=mesh, in_specs=placed, out_specs=P("layer", None, None, "leaf"), check_vma=False,
    )
```
